256 devices in a mesh: lat: 64 (over x_lo, z, y), dp: 4 (over x_hi, core).
Axes of the slice: x: 4 (x_hi: 2, x_lo: 2; x = x_hi * 2 + x_lo), y: 4, z: 8, core: 2. Of those that a mesh axis runs over, the one named last changes fastest.
Arguments:
- state: float32 [4, 128, 256, 128], P('dp', 'lat'), may hold values from -6 to 6
- cotangent: float32 [4, 128, 256, 128], P('dp', 'lat'), may hold values from -0.18 to 0.18
- w_first: bfloat16 [128, 1024], replicated, may hold values from -0.5 to 0.5
- w_middle: bfloat16 [1024, 1024], replicated, may hold values from -0.1875 to 0.1875
- w_last: bfloat16 [1024, 128], replicated, may hold values from -0.1875 to 0.1875
Outputs:
- final_state: float32 [4, 128, 256, 128], P('dp', 'lat')
- grad_first: float32 [128, 1024], replicated
- grad_middle: float32 [1024, 1024], replicated
- grad_last: float32 [1024, 128], replicated
The draws below stay inside these ranges and needn't reach their ends.
All inputs are finite; a program needn't handle non-finite values.
Results may differ from the reference program's by a relative error of at most 0.0048.
Values sent between devices are 32-bit elements; how exact they have to be, the bound alone decides.
A program may use at most 64 MiB of HBM per device.

```python
import math
import jax
import jax.numpy as jnp
from jax import lax

NLAT = 128
NLON = 256
MW = 64
FEAT = 128
HID = 1024
STEPS = 2
BATCH = 4


def shard_levels(stream_key, dims, cuts, least, top_value):
    factor_of = 1.0
    for position, blocks in cuts:
        heights = jax.random.uniform(jax.random.fold_in(jax.random.fold_in(stream_key, 6), position), (blocks,), jnp.float32, least / len(cuts), top_value / len(cuts))
        factor_of = factor_of * jnp.repeat(jnp.exp(heights), dims[position] // blocks).reshape((-1,) + (1,) * (len(dims) - 1 - position))
    return factor_of


def bell_draw(key, dims, width, most, split=(), held_as=jnp.bfloat16):
    level = shard_levels(key, dims, split, -0.22, 0.18) if split else 1.0
    values = jax.random.normal(key, dims, jnp.float32) * width * level
    return jnp.minimum(jnp.maximum(values, -most), most).astype(held_as)


def setup_inputs(seed: int = 0) -> dict:
    seeds = jax.random.split(jax.random.key(seed), 6)
    return {
        "state": bell_draw(seeds[0], (BATCH, NLAT, NLON, FEAT), 1.0, 6.0, ((0, 4), (1, 64)), jnp.float32),
        "cotangent": bell_draw(seeds[1], (BATCH, NLAT, NLON, FEAT), 0.03, 0.18, ((0, 4), (1, 64)), jnp.float32),
        "w_first": bell_draw(seeds[2], (FEAT, HID), FEAT ** -0.5, 0.5),
        "w_middle": bell_draw(seeds[3], (HID, HID), HID ** -0.5, 0.1875),
        "w_last": bell_draw(seeds[4], (HID, FEAT), HID ** -0.5, 0.1875),
    }


highest = lax.Precision.HIGHEST
tend_weight = 0.5

def grid_tables(lon_count, wave_count):
    lon_index = jnp.arange(lon_count, dtype=jnp.int32)
    wave_index = jnp.arange(wave_count, dtype=jnp.int32)
    phase_angle = (lon_index[:, None] * wave_index[None, :] % lon_count).astype(jnp.float32) * (2.0 * math.pi / lon_count)
    cosine = jnp.cos(phase_angle)
    sine_part = jnp.sin(phase_angle)
    analysis = jnp.stack([cosine, -sine_part], axis=2) / lon_count
    factor = jnp.where(wave_index == 0, 1.0, 2.0).astype(jnp.float32)
    synthesis = jnp.stack([cosine, -sine_part], axis=2) * factor[None, :, None]
    return (analysis, synthesis)

def legendre(wave_ids, lat_count, wave_count):
    lat_index = jnp.arange(lat_count).astype(jnp.float32)
    latitude = (lat_index + 0.5) * (math.pi / lat_count) - 0.5 * math.pi
    sine_lat = jnp.sin(latitude)
    cosine_lat = jnp.cos(latitude)
    quad_weight = cosine_lat * (math.pi / lat_count)
    order_m = wave_ids.astype(jnp.float32)
    counter = jnp.arange(1, wave_count).astype(jnp.float32)
    increments = 0.5 * jnp.log((2.0 * counter + 1.0) / (2.0 * counter))
    summed = lax.optimization_barrier(jnp.sum(jnp.where(counter[None, :] <= order_m[:, None], increments[None, :], 0.0), axis=1))
    diagonal = jnp.exp(0.5 * math.log(0.5) + summed[:, None] + order_m[:, None] * jnp.log(cosine_lat)[None, :])

    def advance(carry, offset):
        previous, current, ratio_prev = carry
        degree = order_m + offset
        ratio_new = jnp.sqrt((4.0 * degree * degree - 1.0) / (degree * degree - order_m * order_m))
        following = ratio_new[:, None] * (sine_lat[None, :] * current - previous / ratio_prev[:, None])
        return ((current, following, ratio_new), following)
    initial = (jnp.zeros_like(diagonal), diagonal, jnp.ones_like(order_m))
    _, remaining = lax.scan(advance, initial, jnp.arange(1, wave_count).astype(jnp.float32))
    poly_table = jnp.concatenate([diagonal[None], remaining], axis=0).transpose(1, 0, 2)
    degree = order_m[:, None] + jnp.arange(wave_count).astype(jnp.float32)[None, :]
    kept_mask = degree <= wave_count - 1
    poly_table = jnp.where(kept_mask[:, :, None], poly_table, 0.0)
    damping = jnp.where(kept_mask, 1.0 / (1.0 + degree * (degree + 1.0) / (wave_count * (wave_count - 1.0))), 0.0)
    return (poly_table, quad_weight, damping)

def spectral_whole(field, first, last, in_table, out_table, damping):
    wave_grid = jnp.einsum('bjxf,xmp->bjmpf', field, first, precision=highest)
    coeffs = jnp.einsum('mkj,bjmpf->bmkpf', in_table, wave_grid, precision=highest) * damping[None, :, :, None, None]
    back_grid = jnp.einsum('mkj,bmkpf->bjmpf', out_table, coeffs, precision=highest)
    return jnp.einsum('bjmpf,xmp->bjxf', back_grid, last, precision=highest)

def silu_slope(value):
    gate_sig = jax.nn.sigmoid(value)
    return gate_sig * (1.0 + value * (1.0 - gate_sig))

def hidden_rows(rows, w_first, w_middle):
    pre_first = jnp.dot(rows, w_first, preferred_element_type=jnp.float32)
    hidden_first = jax.nn.silu(pre_first).astype(jnp.bfloat16)
    pre_middle = jnp.dot(hidden_first, w_middle, preferred_element_type=jnp.float32)
    hidden_middle = jax.nn.silu(pre_middle).astype(jnp.bfloat16)
    return (pre_first, hidden_first, pre_middle, hidden_middle)

def forward_rows(rows, w_first, w_middle, w_last):
    _, _, _, hidden_middle = hidden_rows(rows, w_first, w_middle)
    return jnp.dot(hidden_middle, w_last, preferred_element_type=jnp.float32)

def backward_rows(rows, scaled, w_first, w_middle, w_last):
    pre_first, hidden_first, pre_middle, hidden_middle = hidden_rows(rows, w_first, w_middle)
    grad_last = jnp.dot(hidden_middle.T, scaled, preferred_element_type=jnp.float32)
    middle_back = jnp.dot(scaled, w_last.T, preferred_element_type=jnp.float32)
    middle_grad = (middle_back * silu_slope(pre_middle)).astype(jnp.bfloat16)
    grad_middle = jnp.dot(hidden_first.T, middle_grad, preferred_element_type=jnp.float32)
    first_back = jnp.dot(middle_grad, w_middle.T, preferred_element_type=jnp.float32)
    first_grad = (first_back * silu_slope(pre_first)).astype(jnp.bfloat16)
    grad_first = jnp.dot(rows.T, first_grad, preferred_element_type=jnp.float32)
    back_rows = jnp.dot(first_grad, w_first.T, preferred_element_type=jnp.float32)
    return ((grad_first, grad_middle, grad_last), back_rows)

def reference(state, cotangent, w_first, w_middle, w_last):
    batch, lat_count, lon_count, features = state.shape
    hidden_count = w_first.shape[1]
    analysis, synthesis = grid_tables(lon_count, MW)
    poly_table, quad_weight, damping = legendre(jnp.arange(MW, dtype=jnp.int32), lat_count, MW)
    weighted = poly_table * quad_weight[None, None, :]
    row_count = batch * lat_count * lon_count
    block = math.gcd(row_count, 8192)
    inputs = []
    field = state
    for step_index in range(STEPS):
        inputs.append(field)
        rows = field.reshape(row_count // block, block, features).astype(jnp.bfloat16)
        tendency = lax.map(lambda piece: forward_rows(piece, w_first, w_middle, w_last), rows)
        moved = field + tend_weight * tendency.reshape(field.shape)
        field = spectral_whole(moved, analysis, synthesis, weighted, poly_table, damping)
    final_state = field
    grad = cotangent
    totals = (jnp.zeros((features, hidden_count), jnp.float32), jnp.zeros((hidden_count, hidden_count), jnp.float32), jnp.zeros((hidden_count, features), jnp.float32))
    for step_index in reversed(range(STEPS)):
        pulled = spectral_whole(grad, synthesis, analysis, poly_table, weighted, damping)
        scaled = (tend_weight * pulled).astype(jnp.bfloat16).reshape(row_count // block, block, features)
        rows = inputs[step_index].reshape(row_count // block, block, features).astype(jnp.bfloat16)

        def accumulate(carry, pieces):
            grads, back_rows = backward_rows(pieces[0], pieces[1], w_first, w_middle, w_last)
            return ((carry[0] + grads[0], carry[1] + grads[1], carry[2] + grads[2]), back_rows)
        totals, back_rows = lax.scan(accumulate, totals, (rows, scaled))
        grad = pulled + back_rows.reshape(field.shape)
    return (final_state, totals[0], totals[1], totals[2])
```

```python
import functools
import math

import jax
import jax.numpy as jnp
import numpy as np
from jax import lax
from jax.experimental import pallas as pl
from jax.experimental.pallas import tpu as pltpu
from jax.sharding import PartitionSpec as P

MW = 64
NLAT = 128
NLON = 256
FEAT = 128
HID = 1024
ROWS = 512
BANDS = 64
BLK = 1280
BF = jnp.bfloat16
F32 = jnp.float32
MESH = pl.DeviceIdType.MESH


def split_terms(table):
    high = table.astype(np.float32).astype(np.dtype(BF))
    low = (table - high.astype(np.float64)).astype(np.float32).astype(np.dtype(BF))
    return np.concatenate([high, high, low], axis=1)


@functools.lru_cache(maxsize=None)
def constant_tables():
    lon = np.arange(NLON)
    wave = np.arange(MW)
    angle = 2.0 * math.pi * ((wave[:, None] * lon[None, :]) % NLON) / NLON
    base = np.concatenate([np.cos(angle), -np.sin(angle)], axis=0)
    factor = np.where(wave == 0, 1.0, 2.0)
    analysis = base / NLON
    synthesis = base * np.concatenate([factor, factor])[:, None]
    to_waves = np.stack([split_terms(analysis), split_terms(synthesis)])
    to_grid = np.stack([split_terms(synthesis.T), split_terms(analysis.T)])

    latitude = (np.arange(NLAT) + 0.5) * (math.pi / NLAT) - 0.5 * math.pi
    mu, cosine = np.sin(latitude), np.cos(latitude)
    quad = cosine * (math.pi / NLAT)
    table = np.zeros((MW, MW + 8, NLAT))
    for m in range(MW):
        steps = np.arange(1, m + 1)
        increments = 0.5 * np.log((2.0 * steps + 1.0) / (2.0 * steps))
        current = np.exp(0.5 * math.log(0.5) + increments.sum() + m * np.log(cosine))
        previous, ratio_prev = np.zeros(NLAT), 1.0
        table[m, 0] = current
        for k in range(1, MW - m):
            n = float(m + k)
            ratio = math.sqrt((4.0 * n * n - 1.0) / (n * n - m * m))
            previous, current = current, ratio * (mu * current - previous / ratio_prev)
            ratio_prev = ratio
            table[m, k] = current
    table = np.concatenate([table[:, :, 0::2], table[:, :, 1::2]], axis=2)
    table[:, MW, :] = quad[0::2][:, None]
    table[:, MW + 1, :] = quad[1::2][:, None]
    return to_waves, to_grid, table.astype(np.float32)


def times(table, value):
    high = value.astype(BF)
    low = (value - high.astype(F32)).astype(BF)
    return jnp.dot(table, jnp.concatenate([high, low, high], axis=0), preferred_element_type=F32)


def terms(table):
    high = table.astype(BF)
    low = (table - high.astype(F32)).astype(BF)
    return jnp.concatenate([high, high, low], axis=1)


def nt(a, b):
    return lax.dot_general(a, b, (((1,), (1,)), ((), ())), preferred_element_type=F32)


def tn(a, b):
    return lax.dot_general(a, b, (((0,), (0,)), ((), ())), preferred_element_type=F32)


def spread(send, waves, kind):
    for lat in range(2):
        for part in range(2):
            send[pl.ds(kind * 4 + lat * 2 + part, BANDS, stride=8), :] = waves[
                part * MW : (part + 1) * MW, lat * FEAT : (lat + 1) * FEAT
            ]


def gather_parts(recv, kind):
    return jnp.concatenate(
        [
            jnp.concatenate(
                [recv[pl.ds(kind * 4 + lat * 2 + part, BANDS, stride=8), :] for lat in range(2)],
                axis=1,
            )
            for part in range(2)
        ],
        axis=0,
    )


def kernel(
    state, cot, w1, w2, w3, tab, tf, ti,
    final, total,
    grads, field, x0, x1, gt, ha0, hb0, da0, db0, ha1, hb1, da1, db1, ga, gb,
    send, recv, core_buf, half_buf, z_buf,
    a2a_send, a2a_recv, core_send, core_recv, rs_send, rs_recv, z_send, z_recv,
):
    me = lax.axis_index("lat")
    dp = lax.axis_index("dp")
    xh, core = dp // 2, lax.rem(dp, 2)
    xl, zy = me // 32, lax.rem(me, 32)
    z, y = zy // 4, lax.rem(zy, 4)
    yh, yl = y // 2, lax.rem(y, 2)
    mate = {"lat": me, "dp": xh * 2 + 1 - core}
    partner = {
        "xa": {"lat": (1 - xl) * 32 + zy, "dp": dp},
        "xb": {"lat": (1 - xl) * 32 + zy, "dp": (1 - xh) * 2 + core},
        "ya": {"lat": xl * 32 + z * 4 + yh * 2 + 1 - yl, "dp": dp},
        "yb": {"lat": xl * 32 + z * 4 + 3 - y, "dp": dp},
    }
    bit = {"xa": lax.rem(xl + xh, 2), "xb": xh, "ya": lax.rem(yl + yh, 2), "yb": yh}

    barrier = pltpu.get_barrier_semaphore()

    def greet(j, carry):
        pl.semaphore_signal(
            barrier, inc=1, device_id={"lat": lax.rem(me + j, BANDS), "dp": dp}, device_id_type=MESH
        )
        return carry

    lax.fori_loop(1, BANDS, greet, 0)
    for other in (mate, partner["xb"]):
        pl.semaphore_signal(barrier, inc=1, device_id=other, device_id_type=MESH)

    def forward(lat, x, source, ha, hb, da, db):
        rows = pl.ds(pl.multiple_of(lat * NLON, NLON), NLON)
        mine = x[rows, :]
        for layer in range(2):
            weight, act, slope = ((w1, ha, da), (w2, hb, db))[layer]
            rows_in = mine if layer == 0 else ha[rows, :]
            for n in range(4):
                cols = slice(n * 256, (n + 1) * 256)
                pre = jnp.dot(rows_in, weight[:, cols], preferred_element_type=F32)
                gate = jax.nn.sigmoid(pre)
                out = pre * gate
                act[rows, cols] = out.astype(BF)
                slope[rows, cols] = gate * (1.0 + pre * (1.0 - gate))
        tend = jnp.dot(hb[rows, :], w3[...], preferred_element_type=F32)
        field[rows, :] = source[rows, :] + 0.5 * tend

    def backward(lat, da, db, pulled, want_rows):
        rows = pl.ds(pl.multiple_of(lat * NLON, NLON), NLON)
        scaled = gt[rows, :]
        for n in range(4):
            cols = slice(n * 256, (n + 1) * 256)
            gb[rows, cols] = (nt(scaled, w3[cols, :]) * db[rows, cols]).astype(BF)
        grad_b = gb[rows, :]
        for n in range(4):
            cols = slice(n * 256, (n + 1) * 256)
            ga[rows, cols] = (nt(grad_b, w2[cols, :]) * da[rows, cols]).astype(BF)
        if want_rows:
            pulled[rows, :] = pulled[rows, :] + nt(ga[rows, :], w1[...])

    def weight_grads(x, ha, hb, add):
        def put(start, value):
            for half in range(2):
                block = value[:, half * 128 : (half + 1) * 128]
                rows = pl.ds(pl.multiple_of(start + half * BLK, 128), block.shape[0])
                grads[rows, :] = block + grads[rows, :] if add else block

        def middle(i, carry):
            left = ha[:, pl.ds(pl.multiple_of(i * 256, 256), 256)]
            for n in range(4):
                put(2 * n * BLK + i * 256, tn(left, gb[:, n * 256 : (n + 1) * 256]))
            return carry

        lax.fori_loop(0, 4, middle, 0)
        for n in range(4):
            cols = slice(n * 256, (n + 1) * 256)
            put(2 * n * BLK + 1024, tn(x[...], ga[:, cols]))
            put(2 * n * BLK + 1152, tn(gt[...], hb[:, cols]))

    def lanes(ref):
        return jnp.concatenate([ref[0:NLON, :], ref[NLON : 2 * NLON, :]], axis=1)

    quad = jnp.concatenate([tab[MW : MW + 1, :], tab[MW + 1 : MW + 2, :]], axis=1)

    def to_waves(ref, kind, out):
        waves = times(tf[kind], lanes(ref))
        spread(out, waves * quad if kind == 0 else waves, kind)

    def to_grid(source, kind):
        value = times(ti[kind], gather_parts(source, kind))
        return value if kind == 0 else value * quad

    def exchange(index):
        out, into = send.at[index], recv.at[index]
        mine = pl.ds(pl.multiple_of(me * 8, 8), 8)

        def start(j, carry):
            target = lax.rem(me + 18 + j + j // 46, BANDS)
            pltpu.make_async_remote_copy(
                src_ref=out.at[pl.ds(pl.multiple_of(target * 8, 8), 8), :],
                dst_ref=into.at[mine, :],
                send_sem=a2a_send.at[index],
                recv_sem=a2a_recv.at[index],
                device_id={"lat": target, "dp": dp},
                device_id_type=MESH,
            ).start()
            return carry

        lax.fori_loop(0, BANDS - 1, start, 0)
        recv[index, mine, :] = send[index, mine, :]

    def arrive(index):
        most = pl.ds(0, 8 * (BANDS - 1))
        pltpu.make_async_copy(recv.at[index, most, :], recv.at[index, most, :], a2a_recv.at[index]).wait()
        pltpu.make_async_copy(send.at[index, most, :], send.at[index, most, :], a2a_send.at[index]).wait()

    def legendre(source, target):
        degree = me + lax.broadcasted_iota(jnp.int32, (MW, NLAT), 0)
        size = (degree * (degree + 1)).astype(F32)
        damping = jnp.where(degree <= MW - 1, 1.0 / (1.0 + size / (MW * (MW - 1.0))), 0.0)
        poly = tab[0:MW, :]
        columns = [(kind, part) for kind in range(2) for part in range(2)]
        value = jnp.concatenate(
            [
                jnp.concatenate(
                    [source[pl.ds(kind * 4 + lat * 2 + part, BANDS, stride=8), :] for lat in range(2)],
                    axis=0,
                )
                for kind, part in columns
            ],
            axis=1,
        )
        coeffs = times(terms(poly * damping), value)
        back = times(terms(poly.T), coeffs)
        for i, (kind, part) in enumerate(columns):
            for lat in range(2):
                target[pl.ds(kind * 4 + lat * 2 + part, BANDS, stride=8), :] = back[
                    lat * BANDS : (lat + 1) * BANDS, i * FEAT : (i + 1) * FEAT
                ]

    def both(step):
        def run(lat, carry):
            step(lat)
            return carry

        lax.fori_loop(0, 2, run, 0)

    to_waves(cot, 1, send.at[0])
    x0[...] = state[...].astype(BF)
    both(lambda lat: forward(lat, x0, state, ha0, hb0, da0, db0))
    to_waves(field, 0, send.at[0])
    pl.semaphore_wait(barrier, BANDS + 1)
    exchange(0)
    arrive(0)
    legendre(recv.at[0], send.at[1])
    exchange(1)
    arrive(1)

    value = to_grid(recv.at[1], 0)
    pulled = to_grid(recv.at[1], 1)
    for lat in range(2):
        rows, cols = slice(lat * NLON, (lat + 1) * NLON), slice(lat * FEAT, (lat + 1) * FEAT)
        field[rows, :] = value[:, cols]
        x1[rows, :] = value[:, cols].astype(BF)
        final[rows, :] = pulled[:, cols]
        gt[rows, :] = (0.5 * pulled[:, cols]).astype(BF)
    both(lambda lat: forward(lat, x1, field, ha1, hb1, da1, db1))
    to_waves(field, 0, send.at[2])
    both(lambda lat: backward(lat, da1, db1, final, True))
    to_waves(final, 1, send.at[2])
    exchange(2)
    weight_grads(x1, ha1, hb1, False)
    arrive(2)
    legendre(recv.at[2], send.at[3])
    exchange(3)
    arrive(3)

    pulled = to_grid(recv.at[3], 1)
    for lat in range(2):
        rows, cols = slice(lat * NLON, (lat + 1) * NLON), slice(lat * FEAT, (lat + 1) * FEAT)
        gt[rows, :] = (0.5 * pulled[:, cols]).astype(BF)
    both(lambda lat: backward(lat, da0, db0, None, False))
    weight_grads(x0, ha0, hb0, True)
    value = to_grid(recv.at[3], 0)
    for lat in range(2):
        rows, cols = slice(lat * NLON, (lat + 1) * NLON), slice(lat * FEAT, (lat + 1) * FEAT)
        final[rows, :] = value[:, cols]

    def tiles(ref, start, count):
        return ref.at[pl.ds(pl.multiple_of(start * 8, 8), count * 8), :]

    def add(start, source, source_start, count):
        def one(i, carry):
            for j in range(5):
                into = pl.ds(pl.multiple_of((start + i * 5 + j) * 8, 8), 8)
                rows = pl.ds(pl.multiple_of((source_start + i * 5 + j) * 8, 8), 8)
                grads[into, :] = grads[into, :] + source[rows, :]
            return carry

        lax.fori_loop(0, count // 5, one, 0)

    def copy(source, target, send_sem, recv_sem, device):
        return pltpu.make_async_remote_copy(
            src_ref=source, dst_ref=target, send_sem=send_sem, recv_sem=recv_sem,
            device_id=device, device_id_type=MESH,
        )

    order = (
        ("xa", "xb", "ya", "yb"),
        ("xb", "xa", "yb", "ya"),
        ("ya", "yb", "xa", "xb"),
        ("yb", "ya", "xb", "xa"),
    )
    size = 160
    starts = []
    for s in range(4):
        c = copy(
            tiles(grads, (1 - core) * 640 + s * size, size), tiles(core_buf, s * size, size),
            core_send.at[s], core_recv.at[s], mate,
        )
        c.start()
        starts.append(c)
    offset = [core * 640 + s * size for s in range(4)]
    for s in range(4):
        starts[s].wait()
        add(offset[s], core_buf, s * size, size)
    kept = [[o] for o in offset]
    place = 0
    running = {}
    for step in range(5):
        count = size >> (step + 1)
        for s in range(4):
            if step > 0:
                c, keep, base = running[s]
                c.wait()
                add(keep, half_buf, base, count * 2)
                kept[s].append(keep)
            if step < 4:
                name = order[s][step]
                now = kept[s][step]
                keep = now + bit[name] * count
                gone = now + (1 - bit[name]) * count
                c = copy(
                    tiles(grads, gone, count), tiles(half_buf, place, count),
                    rs_send.at[step * 4 + s], rs_recv.at[step * 4 + s], partner[name],
                )
                c.start()
                running[s] = (c, keep, place)
                place += count

    def chunk(index):
        which = index // 2
        start = jnp.where(
            which == 0,
            kept[0][4],
            jnp.where(which == 1, kept[1][4], jnp.where(which == 2, kept[2][4], kept[3][4])),
        )
        return start + 5 * lax.rem(index, 2)

    own = chunk(z)
    zs = []
    for i in range(1, 8):
        other = lax.rem(z + i, 8)
        c = copy(
            tiles(grads, chunk(other), 5), tiles(z_buf, 5 * (i - 1), 5),
            z_send.at[i - 1], z_recv.at[i - 1], {"lat": xl * 32 + other * 4 + y, "dp": dp},
        )
        c.start()
        zs.append(c)
    for c in zs:
        c.wait()
    for j in range(5):
        rows = pl.ds(pl.multiple_of((own + j) * 8, 8), 8)
        value = grads[rows, :]
        for i in range(7):
            value = value + z_buf[(5 * i + j) * 8 : (5 * i + j + 1) * 8, :]
        total[rows, :] = value

    zs = []
    for i in range(1, 8):
        other = lax.rem(z + i, 8)
        c = copy(
            tiles(total, own, 5), tiles(total, own, 5),
            z_send.at[6 + i], z_recv.at[6 + i], {"lat": xl * 32 + other * 4 + y, "dp": dp},
        )
        c.start()
        zs.append(c)
    for c in zs:
        c.wait()
    running = {}
    for step in (3, 2, 1, 0, -1):
        for s in range(4):
            if step < 3:
                running[s].wait()
            if step >= 0:
                count = size >> (step + 1)
                held = tiles(total, kept[s][step + 1], count)
                sem = 16 + step * 4 + s
                c = copy(held, held, rs_send.at[sem], rs_recv.at[sem], partner[order[s][step]])
            else:
                held = tiles(total, offset[s], size)
                c = copy(held, held, core_send.at[4 + s], core_recv.at[4 + s], mate)
            c.start()
            running[s] = c
    for s in range(4):
        running[s].wait()


def body(state, cotangent, w_first, w_middle, w_last):
    to_waves, to_grid, table = constant_tables()
    tab = lax.dynamic_index_in_dim(jnp.asarray(table), lax.axis_index("lat"), 0, keepdims=False)
    vmem = pl.BlockSpec(memory_space=pltpu.VMEM)
    act = pltpu.VMEM((ROWS, HID), BF)
    slope = pltpu.VMEM((ROWS, HID), F32)
    thin = pltpu.VMEM((ROWS, FEAT), BF)
    dma = pltpu.SemaphoreType.DMA
    final, grads = pl.pallas_call(
        kernel,
        out_shape=(
            jax.ShapeDtypeStruct((ROWS, FEAT), F32),
            jax.ShapeDtypeStruct((8 * BLK, 128), F32),
        ),
        in_specs=[vmem] * 8,
        out_specs=(vmem, vmem),
        scratch_shapes=[
            pltpu.VMEM((8 * BLK, 128), F32), pltpu.VMEM((ROWS, FEAT), F32), thin, thin, thin,
            act, act, slope, slope, act, act, slope, slope, act, act,
            pltpu.VMEM((4, 8 * BANDS, FEAT), F32), pltpu.VMEM((4, 8 * BANDS, FEAT), F32),
            pltpu.VMEM((640 * 8, 128), F32), pltpu.VMEM((600 * 8, 128), F32),
            pltpu.VMEM((35 * 8, 128), F32),
            dma((4,)), dma((4,)), dma((8,)), dma((8,)), dma((32,)), dma((32,)), dma((14,)), dma((14,)),
        ],
        compiler_params=pltpu.CompilerParams(
            collective_id=0, has_side_effects=True, vmem_limit_bytes=60 * 1024 * 1024
        ),
        name="spectral_steps",
    )(
        state.reshape(ROWS, FEAT), cotangent.reshape(ROWS, FEAT), w_first, w_middle, w_last,
        tab, jnp.asarray(to_waves), jnp.asarray(to_grid),
    )
    blocks = grads.reshape(8, BLK, 128)

    def columns(piece):
        return piece.transpose(1, 0, 2).reshape(piece.shape[1], HID)

    return (
        final.reshape(state.shape),
        columns(blocks[:, 1024:1152]),
        columns(blocks[:, :1024]),
        columns(blocks[:, 1152:]).T,
    )


def solution(mesh):
    in_specs = (P("dp", "lat", None, None), P("dp", "lat", None, None), P(), P(), P())
    out_specs = (P("dp", "lat", None, None), P(), P(), P())
    return jax.shard_map(body, mesh=mesh, in_specs=in_specs, out_specs=out_specs, check_vma=False)
```

```python
import functools
import math

import jax
import jax.numpy as jnp
import numpy as np
from jax import lax
from jax.experimental import pallas as pl
from jax.experimental.pallas import tpu as pltpu
from jax.sharding import PartitionSpec as P

MW = 64
NLAT = 128
NLON = 256
FEAT = 128
HID = 1024
ROWS = 512
BANDS = 64
BLK = 1280
BF = jnp.bfloat16
F32 = jnp.float32
MESH = pl.DeviceIdType.MESH


def split_terms(table):
    high = table.astype(np.float32).astype(np.dtype(BF))
    low = (table - high.astype(np.float64)).astype(np.float32).astype(np.dtype(BF))
    return np.concatenate([high, high, low], axis=1)


@functools.lru_cache(maxsize=None)
def constant_tables():
    lon = np.arange(NLON)
    wave = np.arange(MW)
    angle = 2.0 * math.pi * ((wave[:, None] * lon[None, :]) % NLON) / NLON
    base = np.concatenate([np.cos(angle), -np.sin(angle)], axis=0)
    factor = np.where(wave == 0, 1.0, 2.0)
    analysis = base / NLON
    synthesis = base * np.concatenate([factor, factor])[:, None]
    to_waves = np.stack([split_terms(analysis), split_terms(synthesis)])
    to_grid = np.stack([split_terms(synthesis.T), split_terms(analysis.T)])

    latitude = (np.arange(NLAT) + 0.5) * (math.pi / NLAT) - 0.5 * math.pi
    mu, cosine = np.sin(latitude), np.cos(latitude)
    quad = cosine * (math.pi / NLAT)
    table = np.zeros((MW, MW, NLAT))
    for m in range(MW):
        steps = np.arange(1, m + 1)
        increments = 0.5 * np.log((2.0 * steps + 1.0) / (2.0 * steps))
        current = np.exp(0.5 * math.log(0.5) + increments.sum() + m * np.log(cosine))
        previous, ratio_prev = np.zeros(NLAT), 1.0
        table[m, 0] = current
        for k in range(1, MW - m):
            n = float(m + k)
            ratio = math.sqrt((4.0 * n * n - 1.0) / (n * n - m * m))
            previous, current = current, ratio * (mu * current - previous / ratio_prev)
            ratio_prev = ratio
            table[m, k] = current
    table = np.concatenate([table[:, :, 0::2], table[:, :, 1::2]], axis=2)
    packed = [table[m, : MW - 8 * (m // 8)] for m in range(MW)] + [np.zeros((MW - 8, NLAT))]
    return to_waves, to_grid, np.concatenate(packed).astype(np.float32), quad.astype(np.float32)


def times(table, value):
    high = value.astype(BF)
    low = (value - high.astype(F32)).astype(BF)
    return jnp.dot(table, jnp.concatenate([high, low, high], axis=0), preferred_element_type=F32)


def terms(table):
    high = table.astype(BF)
    low = (table - high.astype(F32)).astype(BF)
    return jnp.concatenate([high, high, low], axis=1)


def nt(a, b):
    return lax.dot_general(a, b, (((1,), (1,)), ((), ())), preferred_element_type=F32)


def tn(a, b):
    return lax.dot_general(a, b, (((0,), (0,)), ((), ())), preferred_element_type=F32)


def spread(send, waves, kind):
    for lat in range(2):
        for part in range(2):
            send[pl.ds(kind * 4 + lat * 2 + part, BANDS, stride=8), :] = waves[
                part * MW : (part + 1) * MW, lat * FEAT : (lat + 1) * FEAT
            ]


def gather_parts(recv, kind):
    return jnp.concatenate(
        [
            jnp.concatenate(
                [recv[pl.ds(kind * 4 + lat * 2 + part, BANDS, stride=8), :] for lat in range(2)],
                axis=1,
            )
            for part in range(2)
        ],
        axis=0,
    )


def kernel(
    state_in, cot_in, w1_in, w2_in, w3_in, tab_in, tf_in, ti_in, quad_in,
    final, total,
    state, cot, w1, w2, w3, tab, tf, ti,
    grads, field, x0, x1, gt, ha0, hb0, da0, db0, ha1, hb1, da1, db1, ga, gb,
    send, recv, core_buf, half_buf, z_buf,
    loads, a2a_send, a2a_recv, core_send, core_recv, rs_send, rs_recv, z_send, z_recv,
):
    me = lax.axis_index("lat")
    dp = lax.axis_index("dp")
    xh, core = dp // 2, lax.rem(dp, 2)
    xl, zy = me // 32, lax.rem(me, 32)
    z, y = zy // 4, lax.rem(zy, 4)
    yh, yl = y // 2, lax.rem(y, 2)
    mate = {"lat": me, "dp": xh * 2 + 1 - core}
    partner = {
        "xa": {"lat": (1 - xl) * 32 + zy, "dp": dp},
        "xb": {"lat": (1 - xl) * 32 + zy, "dp": (1 - xh) * 2 + core},
        "ya": {"lat": xl * 32 + z * 4 + yh * 2 + 1 - yl, "dp": dp},
        "yb": {"lat": xl * 32 + z * 4 + 3 - y, "dp": dp},
    }
    bit = {"xa": lax.rem(xl + xh, 2), "xb": xh, "ya": lax.rem(yl + yh, 2), "yb": yh}

    group = me // 8
    first_row = 64 * (8 * group - group * (group - 1) // 2) + lax.rem(me, 8) * (8 - group) * 8
    wanted = {
        "cot": (cot_in, cot), "tf": (tf_in, tf), "state": (state_in, state), "w1": (w1_in, w1),
        "w2": (w2_in, w2), "w3": (w3_in, w3), "ti": (ti_in, ti),
        "tab": (tab_in.at[pl.ds(pl.multiple_of(first_row, 8), MW), :], tab),
    }
    loading = {
        name: pltpu.make_async_copy(a, b, loads.at[i]) for i, (name, (a, b)) in enumerate(wanted.items())
    }
    for c in loading.values():
        c.start()

    barrier = pltpu.get_barrier_semaphore()

    def greet(j, carry):
        pl.semaphore_signal(
            barrier, inc=1, device_id={"lat": lax.rem(me + j, BANDS), "dp": dp}, device_id_type=MESH
        )
        return carry

    lax.fori_loop(1, BANDS, greet, 0)
    for other in (mate, partner["xb"]):
        pl.semaphore_signal(barrier, inc=1, device_id=other, device_id_type=MESH)

    def forward(lat, x, source, ha, hb, da, db):
        rows = pl.ds(pl.multiple_of(lat * NLON, NLON), NLON)
        mine = x[rows, :]
        for layer in range(2):
            weight, act, slope = ((w1, ha, da), (w2, hb, db))[layer]
            rows_in = mine if layer == 0 else ha[rows, :]
            for n in range(4):
                cols = slice(n * 256, (n + 1) * 256)
                pre = jnp.dot(rows_in, weight[:, cols], preferred_element_type=F32)
                gate = jax.nn.sigmoid(pre)
                out = pre * gate
                act[rows, cols] = out.astype(BF)
                slope[rows, cols] = gate * (1.0 + pre * (1.0 - gate))
        tend = jnp.dot(hb[rows, :], w3[...], preferred_element_type=F32)
        field[rows, :] = source[rows, :] + 0.5 * tend

    def backward(lat, da, db, pulled, want_rows):
        rows = pl.ds(pl.multiple_of(lat * NLON, NLON), NLON)
        scaled = gt[rows, :]
        for n in range(4):
            cols = slice(n * 256, (n + 1) * 256)
            gb[rows, cols] = (nt(scaled, w3[cols, :]) * db[rows, cols]).astype(BF)
        grad_b = gb[rows, :]
        for n in range(4):
            cols = slice(n * 256, (n + 1) * 256)
            ga[rows, cols] = (nt(grad_b, w2[cols, :]) * da[rows, cols]).astype(BF)
        if want_rows:
            pulled[rows, :] = pulled[rows, :] + nt(ga[rows, :], w1[...])

    def weight_grads(x, ha, hb, add):
        def put(start, value, flip=False):
            for half in range(2):
                block = value[:, half * 128 : (half + 1) * 128]
                block = block.T if flip else block
                rows = pl.ds(pl.multiple_of(start + half * BLK, 128), block.shape[0])
                grads[rows, :] = block + grads[rows, :] if add else block

        def middle(i, carry):
            left = ha[:, pl.ds(pl.multiple_of(i * 256, 256), 256)]
            for n in range(4):
                put(2 * n * BLK + i * 256, tn(left, gb[:, n * 256 : (n + 1) * 256]))
            return carry

        lax.fori_loop(0, 4, middle, 0)
        for n in range(4):
            cols = slice(n * 256, (n + 1) * 256)
            put(2 * n * BLK + 1024, tn(x[...], ga[:, cols]))
            put(2 * n * BLK + 1152, tn(gt[...], hb[:, cols]), True)

    def lanes(ref):
        return jnp.concatenate([ref[0:NLON, :], ref[NLON : 2 * NLON, :]], axis=1)

    quad = jnp.concatenate([jnp.full((1, FEAT), quad_in[2 * me + lat], F32) for lat in range(2)], axis=1)

    def to_waves(ref, kind, out):
        waves = times(tf[kind], lanes(ref))
        spread(out, waves * quad if kind == 0 else waves, kind)

    def to_grid(source, kind):
        value = times(ti[kind], gather_parts(source, kind))
        return value if kind == 0 else value * quad

    def piece(ref, index, device, kind):
        return ref.at[index, pl.ds(pl.multiple_of(device * 8, 8), 8), :].at[pl.ds(4 * kind, 4), :]

    def exchange(index, kind):
        def start(j, carry):
            target = lax.rem(me + 18 + j + j // 46, BANDS)
            pltpu.make_async_remote_copy(
                src_ref=piece(send, index, target, kind),
                dst_ref=piece(recv, index, me, kind),
                send_sem=a2a_send.at[2 * index + kind],
                recv_sem=a2a_recv.at[2 * index + kind],
                device_id={"lat": target, "dp": dp},
                device_id_type=MESH,
            ).start()
            return carry

        lax.fori_loop(0, BANDS - 1, start, 0)
        mine = pl.ds(pl.multiple_of(me * 8, 8) + 4 * kind, 4)
        recv[index, mine, :] = send[index, mine, :]

    def arrive(index, kind):
        most = pl.ds(0, 4 * (BANDS - 1))
        for ref, sem in ((recv, a2a_recv), (send, a2a_send)):
            half = ref.at[index, most, :]
            pltpu.make_async_copy(half, half, sem.at[2 * index + kind]).wait()

    def legendre(source, target, kind):
        degree = me + lax.broadcasted_iota(jnp.int32, (MW, NLAT), 0)
        size = (degree * (degree + 1)).astype(F32)
        damping = jnp.where(degree <= MW - 1, 1.0 / (1.0 + size / (MW * (MW - 1.0))), 0.0)
        poly = tab[...]
        value = jnp.concatenate(
            [
                jnp.concatenate(
                    [source[pl.ds(kind * 4 + lat * 2 + part, BANDS, stride=8), :] for lat in range(2)],
                    axis=0,
                )
                for part in range(2)
            ],
            axis=1,
        )
        coeffs = times(terms(poly * damping), value)
        back = times(terms(poly.T), coeffs)
        for part in range(2):
            for lat in range(2):
                target[pl.ds(kind * 4 + lat * 2 + part, BANDS, stride=8), :] = back[
                    lat * BANDS : (lat + 1) * BANDS, part * FEAT : (part + 1) * FEAT
                ]

    def turn(index, kind):
        arrive(index, kind)
        legendre(recv.at[index], send.at[index + 1], kind)
        exchange(index + 1, kind)

    def both(step):
        def run(lat, carry):
            step(lat)
            return carry

        lax.fori_loop(0, 2, run, 0)

    for name in ("cot", "tf"):
        loading[name].wait()
    to_waves(cot, 1, send.at[0])
    for name in ("state", "w1", "w2", "w3"):
        loading[name].wait()
    x0[...] = state[...].astype(BF)

    def opening(lat):
        forward(lat, x0, state, ha0, hb0, da0, db0)

        @pl.when(lat == 0)
        def _():
            pl.semaphore_wait(barrier, BANDS + 1)
            exchange(0, 1)

    both(opening)
    to_waves(field, 0, send.at[0])
    exchange(0, 0)
    for name in ("ti", "tab"):
        loading[name].wait()
    turn(0, 1)
    turn(0, 0)

    halves = [(slice(lat * NLON, (lat + 1) * NLON), slice(lat * FEAT, (lat + 1) * FEAT)) for lat in range(2)]
    arrive(1, 0)
    value = to_grid(recv.at[1], 0)
    for rows, cols in halves:
        field[rows, :] = value[:, cols]
        x1[rows, :] = value[:, cols].astype(BF)
    both(lambda lat: forward(lat, x1, field, ha1, hb1, da1, db1))
    to_waves(field, 0, send.at[2])
    exchange(2, 0)
    arrive(1, 1)
    pulled = to_grid(recv.at[1], 1)
    for rows, cols in halves:
        final[rows, :] = pulled[:, cols]
        gt[rows, :] = (0.5 * pulled[:, cols]).astype(BF)
    both(lambda lat: backward(lat, da1, db1, final, True))
    to_waves(final, 1, send.at[2])
    exchange(2, 1)
    weight_grads(x1, ha1, hb1, False)
    turn(2, 1)
    turn(2, 0)

    arrive(3, 1)
    pulled = to_grid(recv.at[3], 1)
    for rows, cols in halves:
        gt[rows, :] = (0.5 * pulled[:, cols]).astype(BF)
    both(lambda lat: backward(lat, da0, db0, None, False))
    weight_grads(x0, ha0, hb0, True)

    def tiles(ref, start, count):
        return ref.at[pl.ds(pl.multiple_of(start * 8, 8), count * 8), :]

    def add(start, source, source_start, count):
        def one(i, carry):
            for j in range(5):
                into = pl.ds(pl.multiple_of((start + i * 5 + j) * 8, 8), 8)
                rows = pl.ds(pl.multiple_of((source_start + i * 5 + j) * 8, 8), 8)
                grads[into, :] = grads[into, :] + source[rows, :]
            return carry

        lax.fori_loop(0, count // 5, one, 0)

    def copy(source, target, send_sem, recv_sem, device):
        return pltpu.make_async_remote_copy(
            src_ref=source, dst_ref=target, send_sem=send_sem, recv_sem=recv_sem,
            device_id=device, device_id_type=MESH,
        )

    order = (
        ("xa", "xb", "ya", "yb"),
        ("xb", "xa", "yb", "ya"),
        ("ya", "yb", "xa", "xb"),
        ("yb", "ya", "xb", "xa"),
    )
    size = 80
    parts = range(8)
    starts = []
    for s in parts:
        c = copy(
            tiles(grads, (1 - core) * 640 + s * size, size), tiles(core_buf, s * size, size),
            core_send.at[s], core_recv.at[s], mate,
        )
        c.start()
        starts.append(c)
    arrive(3, 0)
    value = to_grid(recv.at[3], 0)
    for rows, cols in halves:
        final[rows, :] = value[:, cols]
    offset = [core * 640 + s * size for s in parts]
    kept = [[o] for o in offset]
    place = 0
    running = {}
    for step in range(5):
        count = size >> (step + 1)
        for s in parts:
            if step == 0:
                starts[s].wait()
                add(offset[s], core_buf, s * size, size)
            else:
                c, keep, base = running[s]
                c.wait()
                add(keep, half_buf, base, size >> step)
                kept[s].append(keep)
            if step < 4:
                name = order[s % 4][step]
                now = kept[s][step]
                keep = now + bit[name] * count
                gone = now + (1 - bit[name]) * count
                c = copy(
                    tiles(grads, gone, count), tiles(half_buf, place, count),
                    rs_send.at[step * 8 + s], rs_recv.at[step * 8 + s], partner[name],
                )
                c.start()
                running[s] = (c, keep, place)
                place += count

    def chunk(index):
        start = kept[7][4]
        for s in range(7):
            start = jnp.where(index == s, kept[s][4], start)
        return start

    own = chunk(z)
    zs = []
    for i in range(1, 8):
        other = lax.rem(z + i, 8)
        c = copy(
            tiles(grads, chunk(other), 5), tiles(z_buf, 5 * (i - 1), 5),
            z_send.at[i - 1], z_recv.at[i - 1], {"lat": xl * 32 + other * 4 + y, "dp": dp},
        )
        c.start()
        zs.append(c)
    for c in zs:
        c.wait()
    for j in range(5):
        rows = pl.ds(pl.multiple_of((own + j) * 8, 8), 8)
        value = grads[rows, :]
        for i in range(7):
            value = value + z_buf[(5 * i + j) * 8 : (5 * i + j + 1) * 8, :]
        total[rows, :] = value

    zs = []
    for i in range(1, 8):
        other = lax.rem(z + i, 8)
        c = copy(
            tiles(total, own, 5), tiles(total, own, 5),
            z_send.at[6 + i], z_recv.at[6 + i], {"lat": xl * 32 + other * 4 + y, "dp": dp},
        )
        c.start()
        zs.append(c)
    for c in zs:
        c.wait()
    running = {}
    last = []
    for step in (3, 2, 1, 0, -1):
        for s in parts:
            if step < 3:
                running[s].wait()
            if step >= 0:
                count = size >> (step + 1)
                held = tiles(total, kept[s][step + 1], count)
                sem = 32 + step * 8 + s
                c = copy(held, held, rs_send.at[sem], rs_recv.at[sem], partner[order[s % 4][step]])
                c.start()
                running[s] = c
            if step <= 0:
                first = kept[s][1] if step == 0 else 2 * kept[s][0] + size // 2 - kept[s][1]
                held = tiles(total, first, size // 2)
                sem = 16 + 8 * step + s
                c = copy(held, held, core_send.at[8 + sem], core_recv.at[8 + sem], mate)
                c.start()
                last.append(c)
    for c in last:
        c.wait()


def write_out(final, total, field, first, middle, last, sems):
    copies = [(final, field)]
    for c in range(8):
        cols = pl.ds(c * 128, 128)
        copies.append((total.at[pl.ds(c * BLK, 1024), :], middle.at[:, cols]))
        copies.append((total.at[pl.ds(c * BLK + 1024, 128), :], first.at[:, cols]))
        copies.append((total.at[pl.ds(c * BLK + 1152, 128), :], last.at[cols, :]))
    running = [pltpu.make_async_copy(a, b, sems.at[i]) for i, (a, b) in enumerate(copies)]
    for c in running:
        c.start()
    for c in running:
        c.wait()


def body(state, cotangent, w_first, w_middle, w_last):
    to_waves, to_grid, table, quad = constant_tables()
    hbm = pl.BlockSpec(memory_space=pltpu.HBM)
    vmem = pl.BlockSpec(memory_space=pltpu.VMEM)
    act = pltpu.VMEM((ROWS, HID), BF)
    slope = pltpu.VMEM((ROWS, HID), F32)
    thin = pltpu.VMEM((ROWS, FEAT), BF)
    dma = pltpu.SemaphoreType.DMA
    final, total = pl.pallas_call(
        kernel,
        out_shape=(
            pltpu.VMEM((ROWS, FEAT), F32),
            pltpu.VMEM((8 * BLK, 128), F32),
        ),
        in_specs=[hbm] * 8 + [pl.BlockSpec(memory_space=pltpu.SMEM)],
        out_specs=(vmem, vmem),
        scratch_shapes=[
            pltpu.VMEM((ROWS, FEAT), F32), pltpu.VMEM((ROWS, FEAT), F32),
            pltpu.VMEM((FEAT, HID), BF), pltpu.VMEM((HID, HID), BF), pltpu.VMEM((HID, FEAT), BF),
            pltpu.VMEM((MW, NLAT), F32), pltpu.VMEM(to_waves.shape, BF), pltpu.VMEM(to_grid.shape, BF),
            pltpu.VMEM((8 * BLK, 128), F32), pltpu.VMEM((ROWS, FEAT), F32), thin, thin, thin,
            act, act, slope, slope, act, act, slope, slope, act, act,
            pltpu.VMEM((4, 8 * BANDS, FEAT), F32), pltpu.VMEM((4, 8 * BANDS, FEAT), F32),
            pltpu.VMEM((640 * 8, 128), F32), pltpu.VMEM((600 * 8, 128), F32),
            pltpu.VMEM((35 * 8, 128), F32),
            dma((8,)), dma((8,)), dma((8,)), dma((32,)), dma((32,)), dma((64,)), dma((64,)), dma((14,)), dma((14,)),
        ],
        compiler_params=pltpu.CompilerParams(
            collective_id=0, has_side_effects=True, vmem_limit_bytes=57 * 1024 * 1024
        ),
        name="spectral_steps",
    )(
        state.reshape(ROWS, FEAT), cotangent.reshape(ROWS, FEAT), w_first, w_middle, w_last,
        jnp.asarray(table), jnp.asarray(to_waves), jnp.asarray(to_grid), jnp.asarray(quad),
    )
    anywhere = pl.BlockSpec(memory_space=pl.ANY)
    field, first, middle, last = pl.pallas_call(
        write_out,
        out_shape=(
            jax.ShapeDtypeStruct((ROWS, FEAT), F32),
            jax.ShapeDtypeStruct((FEAT, HID), F32),
            jax.ShapeDtypeStruct((HID, HID), F32),
            jax.ShapeDtypeStruct((HID, FEAT), F32),
        ),
        in_specs=[vmem] * 2,
        out_specs=(anywhere,) * 4,
        scratch_shapes=[dma((25,))],
        compiler_params=pltpu.CompilerParams(vmem_limit_bytes=8 * 1024 * 1024),
        name="write_out",
    )(final, total)
    return field.reshape(state.shape), first, middle, last


def solution(mesh):
    in_specs = (P("dp", "lat", None, None), P("dp", "lat", None, None), P(), P(), P())
    out_specs = (P("dp", "lat", None, None), P(), P(), P())
    return jax.shard_map(body, mesh=mesh, in_specs=in_specs, out_specs=out_specs, check_vma=False)
```

```python
import functools
import math

import jax
import jax.numpy as jnp
import numpy as np
from jax import lax
from jax.experimental import pallas as pl
from jax.experimental.pallas import tpu as pltpu
from jax.sharding import PartitionSpec as P

MW = 64
NLAT = 128
NLON = 256
FEAT = 128
HID = 1024
ROWS = 512
BANDS = 64
BLK = 1280
BF = jnp.bfloat16
F32 = jnp.float32
MESH = pl.DeviceIdType.MESH


def split_terms(table):
    high = table.astype(np.float32).astype(np.dtype(BF))
    low = (table - high.astype(np.float64)).astype(np.float32).astype(np.dtype(BF))
    return np.concatenate([high, high, low], axis=1)


@functools.lru_cache(maxsize=None)
def constant_tables():
    lon = np.arange(NLON)
    wave = np.arange(MW)
    angle = 2.0 * math.pi * ((wave[:, None] * lon[None, :]) % NLON) / NLON
    base = np.concatenate([np.cos(angle), -np.sin(angle)], axis=0)
    factor = np.where(wave == 0, 1.0, 2.0)
    analysis = base / NLON
    synthesis = base * np.concatenate([factor, factor])[:, None]
    to_waves = np.stack([split_terms(analysis), split_terms(synthesis)])
    to_grid = np.stack([split_terms(synthesis.T), split_terms(analysis.T)])

    latitude = (np.arange(NLAT) + 0.5) * (math.pi / NLAT) - 0.5 * math.pi
    mu, cosine = np.sin(latitude), np.cos(latitude)
    quad = cosine * (math.pi / NLAT)
    table = np.zeros((MW, MW, NLAT))
    for m in range(MW):
        steps = np.arange(1, m + 1)
        increments = 0.5 * np.log((2.0 * steps + 1.0) / (2.0 * steps))
        current = np.exp(0.5 * math.log(0.5) + increments.sum() + m * np.log(cosine))
        previous, ratio_prev = np.zeros(NLAT), 1.0
        table[m, 0] = current
        for k in range(1, MW - m):
            n = float(m + k)
            ratio = math.sqrt((4.0 * n * n - 1.0) / (n * n - m * m))
            previous, current = current, ratio * (mu * current - previous / ratio_prev)
            ratio_prev = ratio
            table[m, k] = current
    table = np.concatenate([table[:, :, 0::2], table[:, :, 1::2]], axis=2)
    packed = [table[m, : MW - 8 * (m // 8)] for m in range(MW)] + [np.zeros((MW - 8, NLAT))]
    return to_waves, to_grid, np.concatenate(packed).astype(np.float32), quad.astype(np.float32)


def times(table, value):
    high = value.astype(BF)
    low = (value - high.astype(F32)).astype(BF)
    return jnp.dot(table, jnp.concatenate([high, low, high], axis=0), preferred_element_type=F32)


def terms(table):
    high = table.astype(BF)
    low = (table - high.astype(F32)).astype(BF)
    return jnp.concatenate([high, high, low], axis=1)


def nt(a, b):
    return lax.dot_general(a, b, (((1,), (1,)), ((), ())), preferred_element_type=F32)


def tn(a, b):
    return lax.dot_general(a, b, (((0,), (0,)), ((), ())), preferred_element_type=F32)


def spread(send, waves, kind):
    for lat in range(2):
        for part in range(2):
            send[pl.ds(kind * 4 + lat * 2 + part, BANDS, stride=8), :] = waves[
                part * MW : (part + 1) * MW, lat * FEAT : (lat + 1) * FEAT
            ]


def gather_parts(recv, kind):
    return jnp.concatenate(
        [
            jnp.concatenate(
                [recv[pl.ds(kind * 4 + lat * 2 + part, BANDS, stride=8), :] for lat in range(2)],
                axis=1,
            )
            for part in range(2)
        ],
        axis=0,
    )


def kernel(
    state_in, cot_in, w1_in, w2_in, w3_in, tab_in, tf_in, ti_in, quad_in,
    final, total,
    state, cot, w1, w2, w3, tab, tf, ti,
    inward, outward, grads, field, x0, x1, gt, ha0, hb0, da0, db0, ha1, hb1, da1, db1, ga, gb,
    send, recv, core_buf, half_buf, z_buf,
    loads, a2a_send, a2a_recv, core_send, core_recv, rs_send, rs_recv, z_send, z_recv,
):
    me = lax.axis_index("lat")
    dp = lax.axis_index("dp")
    xh, core = dp // 2, lax.rem(dp, 2)
    xl, zy = me // 32, lax.rem(me, 32)
    z, y = zy // 4, lax.rem(zy, 4)
    yh, yl = y // 2, lax.rem(y, 2)
    mate = {"lat": me, "dp": xh * 2 + 1 - core}
    partner = {
        "xa": {"lat": (1 - xl) * 32 + zy, "dp": dp},
        "xb": {"lat": (1 - xl) * 32 + zy, "dp": (1 - xh) * 2 + core},
        "ya": {"lat": xl * 32 + z * 4 + yh * 2 + 1 - yl, "dp": dp},
        "yb": {"lat": xl * 32 + z * 4 + 3 - y, "dp": dp},
    }
    bit = {"xa": lax.rem(xl + xh, 2), "xb": xh, "ya": lax.rem(yl + yh, 2), "yb": yh}

    group = me // 8
    first_row = 64 * (8 * group - group * (group - 1) // 2) + lax.rem(me, 8) * (8 - group) * 8
    wanted = {
        "cot": (cot_in, cot), "tf": (tf_in, tf), "state": (state_in, state), "w1": (w1_in, w1),
        "w2": (w2_in, w2), "w3": (w3_in, w3), "ti": (ti_in, ti),
        "tab": (tab_in.at[pl.ds(pl.multiple_of(first_row, 8), MW), :], tab),
    }
    loading = {
        name: pltpu.make_async_copy(a, b, loads.at[i]) for i, (name, (a, b)) in enumerate(wanted.items())
    }
    for c in loading.values():
        c.start()

    barrier = pltpu.get_barrier_semaphore()

    def greet(j, carry):
        pl.semaphore_signal(
            barrier, inc=1, device_id={"lat": lax.rem(me + j, BANDS), "dp": dp}, device_id_type=MESH
        )
        return carry

    lax.fori_loop(1, BANDS, greet, 0)
    for other in (mate, partner["xb"]):
        pl.semaphore_signal(barrier, inc=1, device_id=other, device_id_type=MESH)

    def forward(lat, x, source, ha, hb, da, db):
        rows = pl.ds(pl.multiple_of(lat * NLON, NLON), NLON)
        mine = x[rows, :]
        for layer in range(2):
            weight, act, slope = ((w1, ha, da), (w2, hb, db))[layer]
            rows_in = mine if layer == 0 else ha[rows, :]
            for n in range(4):
                cols = slice(n * 256, (n + 1) * 256)
                pre = jnp.dot(rows_in, weight[:, cols], preferred_element_type=F32)
                gate = jax.nn.sigmoid(pre)
                out = pre * gate
                act[rows, cols] = out.astype(BF)
                slope[rows, cols] = gate * (1.0 + pre * (1.0 - gate))
        tend = jnp.dot(hb[rows, :], w3[...], preferred_element_type=F32)
        field[rows, :] = source[rows, :] + 0.5 * tend

    def backward_b(lat, db):
        rows = pl.ds(pl.multiple_of(lat * NLON, NLON), NLON)
        scaled = gt[rows, :]
        for n in range(4):
            cols = slice(n * 256, (n + 1) * 256)
            gb[rows, cols] = (nt(scaled, w3[cols, :]) * db[rows, cols]).astype(BF)

    def backward_a(lat, da, pulled):
        rows = pl.ds(pl.multiple_of(lat * NLON, NLON), NLON)
        grad_b = gb[rows, :]
        for n in range(4):
            cols = slice(n * 256, (n + 1) * 256)
            ga[rows, cols] = (nt(grad_b, w2[cols, :]) * da[rows, cols]).astype(BF)
        if pulled is not None:
            pulled[rows, :] = pulled[rows, :] + nt(ga[rows, :], w1[...])

    def put(start, value, add, flip=False):
        for half in range(2):
            block = value[:, half * 128 : (half + 1) * 128]
            block = block.T if flip else block
            rows = pl.ds(pl.multiple_of(start + half * BLK, 128), block.shape[0])
            grads[rows, :] = block + grads[rows, :] if add else block

    def some(half, n):
        return pl.ds(pl.multiple_of(half * 512 + n * 256, 256), 256)

    def middle_grads(half, ha, add):
        def run(i, carry):
            left = ha[:, pl.ds(pl.multiple_of(i * 256, 256), 256)]
            for n in range(2):
                put((half * 4 + 2 * n) * BLK + i * 256, tn(left, gb[:, some(half, n)]), add)
            return carry

        lax.fori_loop(0, 4, run, 0)

    def outer_grads(half, x, hb, add):
        for n in range(2):
            start = (half * 4 + 2 * n) * BLK
            put(start + 1024, tn(x[...], ga[:, some(half, n)]), add)
            put(start + 1152, tn(gt[...], hb[:, some(half, n)]), add, True)

    def lanes(ref):
        return jnp.concatenate([ref[0:NLON, :], ref[NLON : 2 * NLON, :]], axis=1)

    quad = jnp.concatenate([jnp.full((1, FEAT), quad_in[2 * me + lat], F32) for lat in range(2)], axis=1)

    def to_waves(ref, kind, out):
        waves = times(tf[kind], lanes(ref))
        spread(out, waves * quad if kind == 0 else waves, kind)

    def to_grid(source, kind):
        value = times(ti[kind], gather_parts(source, kind))
        return value if kind == 0 else value * quad

    def piece(ref, index, device, kind):
        return ref.at[index, pl.ds(pl.multiple_of(device * 8, 8), 8), :].at[pl.ds(4 * kind, 4), :]

    def exchange(index, kind):
        def start(i, carry):
            for k in range(7):
                j = i * 7 + k
                target = lax.rem(me + 18 + j + j // 46, BANDS)
                pltpu.make_async_remote_copy(
                    src_ref=piece(send, index, target, kind),
                    dst_ref=piece(recv, index, me, kind),
                    send_sem=a2a_send.at[2 * index + kind],
                    recv_sem=a2a_recv.at[2 * index + kind],
                    device_id={"lat": target, "dp": dp},
                    device_id_type=MESH,
                ).start()
            return carry

        lax.fori_loop(0, 9, start, 0)
        mine = pl.ds(pl.multiple_of(me * 8, 8) + 4 * kind, 4)
        recv[index, mine, :] = send[index, mine, :]

    def arrive(index, kind):
        most = pl.ds(0, 4 * (BANDS - 1))
        for ref, sem in ((recv, a2a_recv), (send, a2a_send)):
            half = ref.at[index, most, :]
            pltpu.make_async_copy(half, half, sem.at[2 * index + kind]).wait()

    def legendre_tables():
        degree = me + lax.broadcasted_iota(jnp.int32, (MW, NLAT), 0)
        size = (degree * (degree + 1)).astype(F32)
        damping = jnp.where(degree <= MW - 1, 1.0 / (1.0 + size / (MW * (MW - 1.0))), 0.0)
        poly = tab[...]
        inward[...] = terms(poly * damping)
        outward[...] = terms(poly.T)

    def legendre(source, target, kind):
        value = jnp.concatenate(
            [
                jnp.concatenate(
                    [source[pl.ds(kind * 4 + lat * 2 + part, BANDS, stride=8), :] for lat in range(2)],
                    axis=0,
                )
                for part in range(2)
            ],
            axis=1,
        )
        coeffs = times(inward[...], value)
        back = times(outward[...], coeffs)
        for part in range(2):
            for lat in range(2):
                target[pl.ds(kind * 4 + lat * 2 + part, BANDS, stride=8), :] = back[
                    lat * BANDS : (lat + 1) * BANDS, part * FEAT : (part + 1) * FEAT
                ]

    def turn(index, kind):
        arrive(index, kind)
        legendre(recv.at[index], send.at[index + 1], kind)
        exchange(index + 1, kind)

    def both(step):
        def run(lat, carry):
            step(lat)
            return carry

        lax.fori_loop(0, 2, run, 0)

    for name in ("cot", "tf"):
        loading[name].wait()
    to_waves(cot, 1, send.at[0])
    for name in ("state", "w1", "w2", "w3"):
        loading[name].wait()
    x0[...] = state[...].astype(BF)

    both(lambda lat: forward(lat, x0, state, ha0, hb0, da0, db0))
    to_waves(field, 0, send.at[0])
    pl.semaphore_wait(barrier, BANDS + 1)
    exchange(0, 0)
    exchange(0, 1)
    for name in ("ti", "tab"):
        loading[name].wait()
    legendre_tables()
    turn(0, 0)
    turn(0, 1)

    halves = [(slice(lat * NLON, (lat + 1) * NLON), slice(lat * FEAT, (lat + 1) * FEAT)) for lat in range(2)]
    arrive(1, 0)
    value = to_grid(recv.at[1], 0)
    for rows, cols in halves:
        field[rows, :] = value[:, cols]
        x1[rows, :] = value[:, cols].astype(BF)
    both(lambda lat: forward(lat, x1, field, ha1, hb1, da1, db1))
    to_waves(field, 0, send.at[2])
    exchange(2, 0)
    arrive(1, 1)
    pulled = to_grid(recv.at[1], 1)
    for rows, cols in halves:
        final[rows, :] = pulled[:, cols]
        gt[rows, :] = (0.5 * pulled[:, cols]).astype(BF)
    both(lambda lat: backward_b(lat, db1))
    both(lambda lat: backward_a(lat, da1, final))
    to_waves(final, 1, send.at[2])
    exchange(2, 1)
    for half in range(2):
        middle_grads(half, ha1, False)
        outer_grads(half, x1, hb1, False)
    turn(2, 1)
    turn(2, 0)

    arrive(3, 1)
    pulled = to_grid(recv.at[3], 1)
    for rows, cols in halves:
        gt[rows, :] = (0.5 * pulled[:, cols]).astype(BF)
    both(lambda lat: backward_b(lat, db0))

    def tiles(ref, start, count):
        return ref.at[pl.ds(pl.multiple_of(start * 8, 8), count * 8), :]

    def add(start, source, source_start, count):
        def one(i, carry):
            for j in range(5):
                into = pl.ds(pl.multiple_of((start + i * 5 + j) * 8, 8), 8)
                rows = pl.ds(pl.multiple_of((source_start + i * 5 + j) * 8, 8), 8)
                grads[into, :] = grads[into, :] + source[rows, :]
            return carry

        lax.fori_loop(0, count // 5, one, 0)

    def copy(source, target, send_sem, recv_sem, device):
        return pltpu.make_async_remote_copy(
            src_ref=source, dst_ref=target, send_sem=send_sem, recv_sem=recv_sem,
            device_id=device, device_id_type=MESH,
        )

    order = (
        ("xa", "xb", "ya", "yb"),
        ("xb", "xa", "yb", "ya"),
        ("ya", "yb", "xa", "xb"),
        ("yb", "ya", "xb", "xa"),
    )
    size = 80
    parts = range(8)
    starts = {}

    def to_mate(chosen):
        for s in chosen:
            c = copy(
                tiles(grads, (1 - core) * 640 + s * size, size), tiles(core_buf, s * size, size),
                core_send.at[s], core_recv.at[s], mate,
            )
            c.start()
            starts[s] = c

    middle_grads(1 - core, ha0, True)
    to_mate((0, 2, 4, 6))
    both(lambda lat: backward_a(lat, da0, None))
    outer_grads(1 - core, x0, hb0, True)
    to_mate((1, 3, 5, 7))
    middle_grads(core, ha0, True)
    outer_grads(core, x0, hb0, True)
    offset = [core * 640 + s * size for s in parts]
    def along_z(index):
        return {"lat": xl * 32 + index * 4 + y, "dp": dp}

    def to_owner(s, act):
        @pl.when(z != s)
        def _():
            act(
                copy(
                    tiles(grads, kept[s][4], 5), tiles(z_buf, 5 * z, 5),
                    z_send.at[s], z_recv.at[z], along_z(s),
                )
            )

    def from_owner(index, i):
        held = tiles(total, chunk(index), 5)
        return copy(held, held, z_send.at[8 + i], z_recv.at[8 + index], along_z(lax.rem(z + i, 8)))

    kept = [[o] for o in offset]
    place = 0
    running = {}
    for step in range(5):
        count = size >> (step + 1)
        for s in parts:
            if step == 0:
                starts[s].wait()
                add(offset[s], core_buf, s * size, size)
            else:
                c, keep, base = running[s]
                c.wait()
                add(keep, half_buf, base, size >> step)
                kept[s].append(keep)
            if step == 4:
                to_owner(s, lambda c: c.start())
            if step < 4:
                name = order[s % 4][step]
                now = kept[s][step]
                keep = now + bit[name] * count
                gone = now + (1 - bit[name]) * count
                c = copy(
                    tiles(grads, gone, count), tiles(half_buf, place, count),
                    rs_send.at[step * 8 + s], rs_recv.at[step * 8 + s], partner[name],
                )
                c.start()
                running[s] = (c, keep, place)
                place += count

    def chunk(index):
        start = kept[7][4]
        for s in range(7):
            start = jnp.where(index == s, kept[s][4], start)
        return start

    own = chunk(z)
    arrive(3, 0)
    value = to_grid(recv.at[3], 0)
    for rows, cols in halves:
        final[rows, :] = value[:, cols]
    others = [lax.rem(z + i, 8) for i in range(1, 8)]
    for other in others:
        copy(
            tiles(grads, own, 5), tiles(z_buf, 5 * other, 5), z_send.at[0], z_recv.at[other], along_z(other)
        ).wait_recv()
    for j in range(5):
        rows = pl.ds(pl.multiple_of((own + j) * 8, 8), 8)
        value = grads[rows, :]
        for other in others:
            value = value + z_buf[pl.ds(pl.multiple_of((5 * other + j) * 8, 8), 8), :]
        total[rows, :] = value
    for i in range(1, 8):
        from_owner(z, i).start()
    running = {}
    last = []
    for step in (3, 2, 1, 0, -1):
        for s in parts:
            if step < 3:
                running[s].wait()
            else:

                @pl.when(z != s)
                def _():
                    from_owner(s, 1).wait_recv()

            if step >= 0:
                count = size >> (step + 1)
                held = tiles(total, kept[s][step + 1], count)
                sem = 32 + step * 8 + s
                c = copy(held, held, rs_send.at[sem], rs_recv.at[sem], partner[order[s % 4][step]])
                c.start()
                running[s] = c
            if step <= 0:
                first = kept[s][1] if step == 0 else 2 * kept[s][0] + size // 2 - kept[s][1]
                held = tiles(total, first, size // 2)
                sem = 16 + 8 * step + s
                c = copy(held, held, core_send.at[8 + sem], core_recv.at[8 + sem], mate)
                c.start()
                last.append(c)
    for s in parts:
        to_owner(s, lambda c: c.wait_send())
    for i in range(1, 8):
        from_owner(z, i).wait_send()
    for c in last:
        c.wait()


def write_out(final, total, field, first, middle, last, sems):
    copies = [(final, field)]
    for c in range(8):
        cols = pl.ds(c * 128, 128)
        copies.append((total.at[pl.ds(c * BLK, 1024), :], middle.at[:, cols]))
        copies.append((total.at[pl.ds(c * BLK + 1024, 128), :], first.at[:, cols]))
        copies.append((total.at[pl.ds(c * BLK + 1152, 128), :], last.at[cols, :]))
    running = [pltpu.make_async_copy(a, b, sems.at[i]) for i, (a, b) in enumerate(copies)]
    for c in running:
        c.start()
    for c in running:
        c.wait()


def body(state, cotangent, w_first, w_middle, w_last):
    to_waves, to_grid, table, quad = constant_tables()
    hbm = pl.BlockSpec(memory_space=pltpu.HBM)
    vmem = pl.BlockSpec(memory_space=pltpu.VMEM)
    act = pltpu.VMEM((ROWS, HID), BF)
    slope = pltpu.VMEM((ROWS, HID), F32)
    thin = pltpu.VMEM((ROWS, FEAT), BF)
    dma = pltpu.SemaphoreType.DMA
    final, total = pl.pallas_call(
        kernel,
        out_shape=(
            pltpu.VMEM((ROWS, FEAT), F32),
            pltpu.VMEM((8 * BLK, 128), F32),
        ),
        in_specs=[hbm] * 8 + [pl.BlockSpec(memory_space=pltpu.SMEM)],
        out_specs=(vmem, vmem),
        scratch_shapes=[
            pltpu.VMEM((ROWS, FEAT), F32), pltpu.VMEM((ROWS, FEAT), F32),
            pltpu.VMEM((FEAT, HID), BF), pltpu.VMEM((HID, HID), BF), pltpu.VMEM((HID, FEAT), BF),
            pltpu.VMEM((MW, NLAT), F32), pltpu.VMEM(to_waves.shape, BF), pltpu.VMEM(to_grid.shape, BF),
            pltpu.VMEM((MW, 3 * NLAT), BF), pltpu.VMEM((NLAT, 3 * MW), BF),
            pltpu.VMEM((8 * BLK, 128), F32), pltpu.VMEM((ROWS, FEAT), F32), thin, thin, thin,
            act, act, slope, slope, act, act, slope, slope, act, act,
            pltpu.VMEM((4, 8 * BANDS, FEAT), F32), pltpu.VMEM((4, 8 * BANDS, FEAT), F32),
            pltpu.VMEM((640 * 8, 128), F32), pltpu.VMEM((600 * 8, 128), F32),
            pltpu.VMEM((40 * 8, 128), F32),
            dma((8,)), dma((8,)), dma((8,)), dma((32,)), dma((32,)), dma((64,)), dma((64,)), dma((16,)), dma((16,)),
        ],
        compiler_params=pltpu.CompilerParams(
            collective_id=0, has_side_effects=True, vmem_limit_bytes=57 * 1024 * 1024
        ),
        name="spectral_steps",
    )(
        state.reshape(ROWS, FEAT), cotangent.reshape(ROWS, FEAT), w_first, w_middle, w_last,
        jnp.asarray(table), jnp.asarray(to_waves), jnp.asarray(to_grid), jnp.asarray(quad),
    )
    anywhere = pl.BlockSpec(memory_space=pl.ANY)
    field, first, middle, last = pl.pallas_call(
        write_out,
        out_shape=(
            jax.ShapeDtypeStruct((ROWS, FEAT), F32),
            jax.ShapeDtypeStruct((FEAT, HID), F32),
            jax.ShapeDtypeStruct((HID, HID), F32),
            jax.ShapeDtypeStruct((HID, FEAT), F32),
        ),
        in_specs=[vmem] * 2,
        out_specs=(anywhere,) * 4,
        scratch_shapes=[dma((25,))],
        compiler_params=pltpu.CompilerParams(vmem_limit_bytes=8 * 1024 * 1024),
        name="write_out",
    )(final, total)
    return field.reshape(state.shape), first, middle, last


def solution(mesh):
    in_specs = (P("dp", "lat", None, None), P("dp", "lat", None, None), P(), P(), P())
    out_specs = (P("dp", "lat", None, None), P(), P(), P())
    return jax.shard_map(body, mesh=mesh, in_specs=in_specs, out_specs=out_specs, check_vma=False)
```

```python
import functools
import math

import jax
import jax.numpy as jnp
import numpy as np
from jax import lax
from jax.experimental import pallas as pl
from jax.experimental.pallas import tpu as pltpu
from jax.sharding import PartitionSpec as P

MW = 64
NLAT = 128
NLON = 256
FEAT = 128
HID = 1024
ROWS = 512
BANDS = 64
BLK = 1280
BF = jnp.bfloat16
F32 = jnp.float32
MESH = pl.DeviceIdType.MESH


def split_terms(table):
    high = table.astype(np.float32).astype(np.dtype(BF))
    low = (table - high.astype(np.float64)).astype(np.float32).astype(np.dtype(BF))
    return np.concatenate([high, high, low], axis=1)


@functools.lru_cache(maxsize=None)
def constant_tables():
    lon = np.arange(NLON)
    wave = np.arange(MW)
    angle = 2.0 * math.pi * ((wave[:, None] * lon[None, :]) % NLON) / NLON
    base = np.concatenate([np.cos(angle), -np.sin(angle)], axis=0)
    factor = np.where(wave == 0, 1.0, 2.0)
    analysis = base / NLON
    synthesis = base * np.concatenate([factor, factor])[:, None]
    to_waves = np.stack([split_terms(analysis), split_terms(synthesis)])
    to_grid = np.stack([split_terms(synthesis.T), split_terms(analysis.T)])

    latitude = (np.arange(NLAT) + 0.5) * (math.pi / NLAT) - 0.5 * math.pi
    mu, cosine = np.sin(latitude), np.cos(latitude)
    quad = cosine * (math.pi / NLAT)
    table = np.zeros((MW, MW, NLAT))
    for m in range(MW):
        steps = np.arange(1, m + 1)
        increments = 0.5 * np.log((2.0 * steps + 1.0) / (2.0 * steps))
        current = np.exp(0.5 * math.log(0.5) + increments.sum() + m * np.log(cosine))
        previous, ratio_prev = np.zeros(NLAT), 1.0
        table[m, 0] = current
        for k in range(1, MW - m):
            n = float(m + k)
            ratio = math.sqrt((4.0 * n * n - 1.0) / (n * n - m * m))
            previous, current = current, ratio * (mu * current - previous / ratio_prev)
            ratio_prev = ratio
            table[m, k] = current
    table = np.concatenate([table[:, :, 0::2], table[:, :, 1::2]], axis=2)
    packed = [table[m, : MW - 8 * (m // 8)] for m in range(MW)] + [np.zeros((MW - 8, NLAT))]
    return to_waves, to_grid, np.concatenate(packed).astype(np.float32), quad.astype(np.float32)


def times(table, value):
    high = value.astype(BF)
    low = (value - high.astype(F32)).astype(BF)
    return jnp.dot(table, jnp.concatenate([high, low, high], axis=0), preferred_element_type=F32)


def terms(table):
    high = table.astype(BF)
    low = (table - high.astype(F32)).astype(BF)
    return jnp.concatenate([high, high, low], axis=1)


def nt(a, b):
    return lax.dot_general(a, b, (((1,), (1,)), ((), ())), preferred_element_type=F32)


def tn(a, b):
    return lax.dot_general(a, b, (((0,), (0,)), ((), ())), preferred_element_type=F32)


def spread(send, waves, kind):
    for lat in range(2):
        for part in range(2):
            send[pl.ds(kind * 4 + lat * 2 + part, BANDS, stride=8), :] = waves[
                part * MW : (part + 1) * MW, lat * FEAT : (lat + 1) * FEAT
            ]


def gather_parts(recv, kind):
    return jnp.concatenate(
        [
            jnp.concatenate(
                [recv[pl.ds(kind * 4 + lat * 2 + part, BANDS, stride=8), :] for lat in range(2)],
                axis=1,
            )
            for part in range(2)
        ],
        axis=0,
    )


def kernel(
    state_in, cot_in, w1_in, w2_in, w3_in, tab_in, tf_in, ti_in, quad_in,
    final, total,
    state, cot, w1, w2, w3, tab, tf, ti,
    inward, outward, grads, field, x0, x1, gt, ha0, hb0, da0, db0, ha1, hb1, da1, db1, ga, gb,
    send, recv, core_buf, half_buf, z_buf,
    loads, a2a_send, a2a_recv, core_send, core_recv, rs_send, rs_recv, z_send, z_recv,
):
    me = lax.axis_index("lat")
    dp = lax.axis_index("dp")
    xh, core = dp // 2, lax.rem(dp, 2)
    xl, zy = me // 32, lax.rem(me, 32)
    z, y = zy // 4, lax.rem(zy, 4)
    yh, yl = y // 2, lax.rem(y, 2)
    mate = {"lat": me, "dp": xh * 2 + 1 - core}
    partner = {
        "xa": {"lat": (1 - xl) * 32 + zy, "dp": dp},
        "xb": {"lat": (1 - xl) * 32 + zy, "dp": (1 - xh) * 2 + core},
        "ya": {"lat": xl * 32 + z * 4 + yh * 2 + 1 - yl, "dp": dp},
        "yb": {"lat": xl * 32 + z * 4 + 3 - y, "dp": dp},
    }
    bit = {"xa": lax.rem(xl + xh, 2), "xb": xh, "ya": lax.rem(yl + yh, 2), "yb": yh}

    def partners(act):
        def run(first, width):
            def inner(i, carry):
                for k in range(width):
                    act(lax.rem(me + (first + i * width + k), BANDS))
                return carry

            return inner

        lax.fori_loop(0, 4, run(44, 5), 0)
        lax.fori_loop(0, 6, run(1, 7), 0)
        act(lax.rem(me + 43, BANDS))

    barrier = pltpu.get_barrier_semaphore()
    partners(
        lambda target: pl.semaphore_signal(
            barrier, inc=1, device_id={"lat": target, "dp": dp}, device_id_type=MESH
        )
    )
    for other in (mate, partner["xb"]):
        pl.semaphore_signal(barrier, inc=1, device_id=other, device_id_type=MESH)

    group = me // 8
    first_row = 64 * (8 * group - group * (group - 1) // 2) + lax.rem(me, 8) * (8 - group) * 8
    wanted = {
        "cot": (cot_in, cot), "tf": (tf_in, tf), "state": (state_in, state), "w1": (w1_in, w1),
        "w2": (w2_in, w2), "w3": (w3_in, w3), "ti": (ti_in, ti),
        "tab": (tab_in.at[pl.ds(pl.multiple_of(first_row, 8), MW), :], tab),
    }
    loading = {
        name: pltpu.make_async_copy(a, b, loads.at[i]) for i, (name, (a, b)) in enumerate(wanted.items())
    }
    for c in loading.values():
        c.start()

    def forward(lat, x, source, ha, hb, da, db):
        rows = pl.ds(pl.multiple_of(lat * NLON, NLON), NLON)
        mine = x[rows, :]
        for layer in range(2):
            weight, act, slope = ((w1, ha, da), (w2, hb, db))[layer]
            rows_in = mine if layer == 0 else ha[rows, :]
            for n in range(4):
                cols = slice(n * 256, (n + 1) * 256)
                pre = jnp.dot(rows_in, weight[:, cols], preferred_element_type=F32)
                gate = jax.nn.sigmoid(pre)
                out = pre * gate
                act[rows, cols] = out.astype(BF)
                slope[rows, cols] = gate * (1.0 + pre * (1.0 - gate))
        tend = jnp.dot(hb[rows, :], w3[...], preferred_element_type=F32)
        field[rows, :] = source[rows, :] + 0.5 * tend

    def backward_b(lat, db):
        rows = pl.ds(pl.multiple_of(lat * NLON, NLON), NLON)
        scaled = gt[rows, :]
        for n in range(4):
            cols = slice(n * 256, (n + 1) * 256)
            gb[rows, cols] = (nt(scaled, w3[cols, :]) * db[rows, cols]).astype(BF)

    def backward_a(lat, da, pulled):
        rows = pl.ds(pl.multiple_of(lat * NLON, NLON), NLON)
        grad_b = gb[rows, :]
        for n in range(4):
            cols = slice(n * 256, (n + 1) * 256)
            ga[rows, cols] = (nt(grad_b, w2[cols, :]) * da[rows, cols]).astype(BF)
        if pulled is not None:
            pulled[rows, :] = pulled[rows, :] + nt(ga[rows, :], w1[...])

    def put(start, value, add, flip=False):
        for half in range(2):
            block = value[:, half * 128 : (half + 1) * 128]
            block = block.T if flip else block
            rows = pl.ds(pl.multiple_of(start + half * BLK, 128), block.shape[0])
            grads[rows, :] = block + grads[rows, :] if add else block

    def some(half, n):
        return pl.ds(pl.multiple_of(half * 512 + n * 256, 256), 256)

    def middle_grads(half, ha, add):
        def run(i, carry):
            left = ha[:, pl.ds(pl.multiple_of(i * 256, 256), 256)]
            for n in range(2):
                put((half * 4 + 2 * n) * BLK + i * 256, tn(left, gb[:, some(half, n)]), add)
            return carry

        lax.fori_loop(0, 4, run, 0)

    def outer_grads(half, x, hb, add):
        for n in range(2):
            start = (half * 4 + 2 * n) * BLK
            put(start + 1024, tn(x[...], ga[:, some(half, n)]), add)
            put(start + 1152, tn(gt[...], hb[:, some(half, n)]), add, True)

    def lanes(ref):
        return jnp.concatenate([ref[0:NLON, :], ref[NLON : 2 * NLON, :]], axis=1)

    quad = jnp.concatenate([jnp.full((1, FEAT), quad_in[2 * me + lat], F32) for lat in range(2)], axis=1)

    def to_waves(ref, kind, out):
        waves = times(tf[kind], lanes(ref))
        spread(out, waves * quad if kind == 0 else waves, kind)

    def to_grid(source, kind):
        value = times(ti[kind], gather_parts(source, kind))
        return value if kind == 0 else value * quad

    def piece(ref, index, device, kind):
        return ref.at[index, pl.ds(pl.multiple_of(device * 8, 8), 8), :].at[pl.ds(4 * kind, 4), :]

    def exchange(index, kind):
        def start(target):
            pltpu.make_async_remote_copy(
                src_ref=piece(send, index, target, kind),
                dst_ref=piece(recv, index, me, kind),
                send_sem=a2a_send.at[2 * index + kind],
                recv_sem=a2a_recv.at[2 * index + kind],
                device_id={"lat": target, "dp": dp},
                device_id_type=MESH,
            ).start()

        partners(start)
        mine = pl.ds(pl.multiple_of(me * 8, 8) + 4 * kind, 4)
        recv[index, mine, :] = send[index, mine, :]

    def arrive(index, kind):
        most = pl.ds(0, 4 * (BANDS - 1))
        for ref, sem in ((recv, a2a_recv), (send, a2a_send)):
            half = ref.at[index, most, :]
            pltpu.make_async_copy(half, half, sem.at[2 * index + kind]).wait()

    def legendre_tables():
        degree = me + lax.broadcasted_iota(jnp.int32, (MW, NLAT), 0)
        size = (degree * (degree + 1)).astype(F32)
        damping = jnp.where(degree <= MW - 1, 1.0 / (1.0 + size / (MW * (MW - 1.0))), 0.0)
        poly = tab[...]
        inward[...] = terms(poly * damping)
        outward[...] = terms(poly.T)

    def legendre(source, target, kind):
        value = jnp.concatenate(
            [
                jnp.concatenate(
                    [source[pl.ds(kind * 4 + lat * 2 + part, BANDS, stride=8), :] for lat in range(2)],
                    axis=0,
                )
                for part in range(2)
            ],
            axis=1,
        )
        coeffs = times(inward[...], value)
        back = times(outward[...], coeffs)
        for part in range(2):
            for lat in range(2):
                target[pl.ds(kind * 4 + lat * 2 + part, BANDS, stride=8), :] = back[
                    lat * BANDS : (lat + 1) * BANDS, part * FEAT : (part + 1) * FEAT
                ]

    def turn(index, kind):
        arrive(index, kind)
        legendre(recv.at[index], send.at[index + 1], kind)
        exchange(index + 1, kind)

    def both(step):
        def run(lat, carry):
            step(lat)
            return carry

        lax.fori_loop(0, 2, run, 0)

    for name in ("cot", "tf"):
        loading[name].wait()
    to_waves(cot, 1, send.at[0])
    for name in ("state", "w1", "w2", "w3"):
        loading[name].wait()
    x0[...] = state[...].astype(BF)

    both(lambda lat: forward(lat, x0, state, ha0, hb0, da0, db0))
    to_waves(field, 0, send.at[0])
    pl.semaphore_wait(barrier, BANDS + 1)
    exchange(0, 0)
    exchange(0, 1)
    for name in ("ti", "tab"):
        loading[name].wait()
    legendre_tables()
    turn(0, 0)
    turn(0, 1)

    halves = [(slice(lat * NLON, (lat + 1) * NLON), slice(lat * FEAT, (lat + 1) * FEAT)) for lat in range(2)]
    arrive(1, 0)
    value = to_grid(recv.at[1], 0)
    for rows, cols in halves:
        field[rows, :] = value[:, cols]
        x1[rows, :] = value[:, cols].astype(BF)
    both(lambda lat: forward(lat, x1, field, ha1, hb1, da1, db1))
    arrive(1, 1)
    pulled = to_grid(recv.at[1], 1)
    for rows, cols in halves:
        final[rows, :] = pulled[:, cols]
        gt[rows, :] = (0.5 * pulled[:, cols]).astype(BF)
    both(lambda lat: backward_b(lat, db1))
    both(lambda lat: backward_a(lat, da1, final))
    to_waves(final, 1, send.at[2])
    exchange(2, 1)
    to_waves(field, 0, send.at[2])
    exchange(2, 0)
    for half in range(2):
        middle_grads(half, ha1, False)
        outer_grads(half, x1, hb1, False)
    turn(2, 1)
    turn(2, 0)

    arrive(3, 1)
    pulled = to_grid(recv.at[3], 1)
    for rows, cols in halves:
        gt[rows, :] = (0.5 * pulled[:, cols]).astype(BF)
    both(lambda lat: backward_b(lat, db0))

    def tiles(ref, start, count):
        return ref.at[pl.ds(pl.multiple_of(start * 8, 8), count * 8), :]

    def add(start, source, source_start, count):
        def one(i, carry):
            for j in range(5):
                into = pl.ds(pl.multiple_of((start + i * 5 + j) * 8, 8), 8)
                rows = pl.ds(pl.multiple_of((source_start + i * 5 + j) * 8, 8), 8)
                grads[into, :] = grads[into, :] + source[rows, :]
            return carry

        lax.fori_loop(0, count // 5, one, 0)

    def copy(source, target, send_sem, recv_sem, device):
        return pltpu.make_async_remote_copy(
            src_ref=source, dst_ref=target, send_sem=send_sem, recv_sem=recv_sem,
            device_id=device, device_id_type=MESH,
        )

    order = (
        ("xa", "xb", "ya", "yb"),
        ("xb", "xa", "yb", "ya"),
        ("ya", "yb", "xa", "xb"),
        ("yb", "ya", "xb", "xa"),
    )
    size = 80
    parts = (0, 2, 4, 6, 1, 3, 5, 7)
    starts = {}

    def to_mate(chosen):
        for s in chosen:
            c = copy(
                tiles(grads, (1 - core) * 640 + s * size, size), tiles(core_buf, s * size, size),
                core_send.at[s], core_recv.at[s], mate,
            )
            c.start()
            starts[s] = c

    offset = {s: core * 640 + s * size for s in parts}
    kept = {s: [offset[s]] for s in parts}
    place = 0
    early, late = {}, {}

    def take(entry):
        c, start, base, count = entry
        c.wait()
        add(start, half_buf, base, count)

    def reduce_step(s, step):
        nonlocal place
        count = size >> (step + 1)
        now = kept[s][step]
        if step >= 2:
            take(late[s, step - 2])
        if step == 0:
            starts[s].wait()
            add(offset[s], core_buf, s * size, size)
        else:
            take(early[s, step - 1])
        if step == 4:
            to_owner(s, lambda c: c.start())
            return
        name = order[s // 2][step]
        keep = now + bit[name] * count
        gone = now + (1 - bit[name]) * count
        kept[s].append(keep)
        if step == 3:
            pieces = [(early, 0, count)]
        else:
            ahead = bit[order[s // 2][step + 1]]
            pieces = [(early, (1 - ahead) * (count // 2), count // 2), (late, ahead * (count // 2), count // 2)]
        for i, (book, at, length) in enumerate(pieces):
            sem = 64 * i + step * 8 + s
            c = copy(
                tiles(grads, gone + at, length), tiles(half_buf, place, length),
                rs_send.at[sem], rs_recv.at[sem], partner[name],
            )
            c.start()
            book[s, step] = (c, keep + at, place, length)
            place += length

    def along_z(index):
        return {"lat": xl * 32 + index * 4 + y, "dp": dp}

    def to_owner(s, act):
        @pl.when(z != s)
        def _():
            act(
                copy(
                    tiles(grads, kept[s][4], 5), tiles(z_buf, 5 * z, 5),
                    z_send.at[s], z_recv.at[z], along_z(s),
                )
            )

    def from_owner(index, i):
        held = tiles(total, chunk(index), 5)
        return copy(held, held, z_send.at[8 + i], z_recv.at[8 + index], along_z(lax.rem(z + i, 8)))

    middle_grads(1 - core, ha0, True)
    to_mate(parts[:4])
    middle_grads(core, ha0, True)
    both(lambda lat: backward_a(lat, da0, None))
    for s in parts[:4]:
        reduce_step(s, 0)
    outer_grads(1 - core, x0, hb0, True)
    to_mate(parts[4:])
    outer_grads(core, x0, hb0, True)
    for s in parts[4:]:
        reduce_step(s, 0)
    for step in range(1, 5):
        for s in parts:
            reduce_step(s, step)

    def chunk(index):
        start = kept[7][4]
        for s in range(7):
            start = jnp.where(index == s, kept[s][4], start)
        return start

    own = chunk(z)
    arrive(3, 0)
    value = to_grid(recv.at[3], 0)
    for rows, cols in halves:
        final[rows, :] = value[:, cols]
    others = [lax.rem(z + i, 8) for i in range(1, 8)]
    for other in others:
        copy(
            tiles(grads, own, 5), tiles(z_buf, 5 * other, 5), z_send.at[0], z_recv.at[other], along_z(other)
        ).wait_recv()
    for j in range(5):
        rows = pl.ds(pl.multiple_of((own + j) * 8, 8), 8)
        value = grads[rows, :]
        for other in others:
            value = value + z_buf[pl.ds(pl.multiple_of((5 * other + j) * 8, 8), 8), :]
        total[rows, :] = value
    for i in range(1, 8):
        from_owner(z, i).start()
    running = {s: [] for s in parts}
    last = []

    def pass_on(s, step, start, length, sem):
        held = tiles(total, start, length)
        c = copy(held, held, rs_send.at[sem], rs_recv.at[sem], partner[order[s // 2][step]])
        c.start()
        running[s].append((step, c))

    for step in (3, 2, 1, 0, -1):
        for s in parts:
            if step < 3:
                for c in [c for at, c in running[s] if at == step + 1]:
                    c.wait()
            else:

                @pl.when(z != s)
                def _():
                    from_owner(s, 1).wait_recv()

            if step == 3:
                pass_on(s, 3, kept[s][4], 5, 56 + s)
            elif step >= 0:
                half = size >> (step + 2)
                pass_on(s, step, 2 * kept[s][step + 1] + half - kept[s][step + 2], half, 32 + step * 8 + s)
            if step >= 1:
                pass_on(s, step - 1, kept[s][step + 1], size >> (step + 1), 88 + (step - 1) * 8 + s)
            if step <= 0:
                first = kept[s][1] if step == 0 else 2 * kept[s][0] + size // 2 - kept[s][1]
                held = tiles(total, first, size // 2)
                sem = 16 + 8 * step + s
                c = copy(held, held, core_send.at[8 + sem], core_recv.at[8 + sem], mate)
                c.start()
                last.append(c)
    for s in parts:
        to_owner(s, lambda c: c.wait_send())
    for i in range(1, 8):
        from_owner(z, i).wait_send()
    for c in last:
        c.wait()


def write_out(final, total, field, first, middle, last, sems):
    copies = [(final, field)]
    for c in range(8):
        cols = pl.ds(c * 128, 128)
        copies.append((total.at[pl.ds(c * BLK, 1024), :], middle.at[:, cols]))
        copies.append((total.at[pl.ds(c * BLK + 1024, 128), :], first.at[:, cols]))
        copies.append((total.at[pl.ds(c * BLK + 1152, 128), :], last.at[cols, :]))
    running = [pltpu.make_async_copy(a, b, sems.at[i]) for i, (a, b) in enumerate(copies)]
    for c in running:
        c.start()
    for c in running:
        c.wait()


def body(state, cotangent, w_first, w_middle, w_last):
    to_waves, to_grid, table, quad = constant_tables()
    hbm = pl.BlockSpec(memory_space=pltpu.HBM)
    vmem = pl.BlockSpec(memory_space=pltpu.VMEM)
    act = pltpu.VMEM((ROWS, HID), BF)
    slope = pltpu.VMEM((ROWS, HID), F32)
    thin = pltpu.VMEM((ROWS, FEAT), BF)
    dma = pltpu.SemaphoreType.DMA
    final, total = pl.pallas_call(
        kernel,
        out_shape=(
            pltpu.VMEM((ROWS, FEAT), F32),
            pltpu.VMEM((8 * BLK, 128), F32),
        ),
        in_specs=[hbm] * 8 + [pl.BlockSpec(memory_space=pltpu.SMEM)],
        out_specs=(vmem, vmem),
        scratch_shapes=[
            pltpu.VMEM((ROWS, FEAT), F32), pltpu.VMEM((ROWS, FEAT), F32),
            pltpu.VMEM((FEAT, HID), BF), pltpu.VMEM((HID, HID), BF), pltpu.VMEM((HID, FEAT), BF),
            pltpu.VMEM((MW, NLAT), F32), pltpu.VMEM(to_waves.shape, BF), pltpu.VMEM(to_grid.shape, BF),
            pltpu.VMEM((MW, 3 * NLAT), BF), pltpu.VMEM((NLAT, 3 * MW), BF),
            pltpu.VMEM((8 * BLK, 128), F32), pltpu.VMEM((ROWS, FEAT), F32), thin, thin, thin,
            act, act, slope, slope, act, act, slope, slope, act, act,
            pltpu.VMEM((4, 8 * BANDS, FEAT), F32), pltpu.VMEM((4, 8 * BANDS, FEAT), F32),
            pltpu.VMEM((640 * 8, 128), F32), pltpu.VMEM((600 * 8, 128), F32),
            pltpu.VMEM((40 * 8, 128), F32),
            dma((8,)), dma((8,)), dma((8,)), dma((32,)), dma((32,)), dma((112,)), dma((112,)), dma((16,)), dma((16,)),
        ],
        compiler_params=pltpu.CompilerParams(
            collective_id=0, has_side_effects=True, vmem_limit_bytes=57 * 1024 * 1024
        ),
        name="spectral_steps",
    )(
        state.reshape(ROWS, FEAT), cotangent.reshape(ROWS, FEAT), w_first, w_middle, w_last,
        jnp.asarray(table), jnp.asarray(to_waves), jnp.asarray(to_grid), jnp.asarray(quad),
    )
    anywhere = pl.BlockSpec(memory_space=pl.ANY)
    field, first, middle, last = pl.pallas_call(
        write_out,
        out_shape=(
            jax.ShapeDtypeStruct((ROWS, FEAT), F32),
            jax.ShapeDtypeStruct((FEAT, HID), F32),
            jax.ShapeDtypeStruct((HID, HID), F32),
            jax.ShapeDtypeStruct((HID, FEAT), F32),
        ),
        in_specs=[vmem] * 2,
        out_specs=(anywhere,) * 4,
        scratch_shapes=[dma((25,))],
        compiler_params=pltpu.CompilerParams(vmem_limit_bytes=8 * 1024 * 1024),
        name="write_out",
    )(final, total)
    return field.reshape(state.shape), first, middle, last


def solution(mesh):
    in_specs = (P("dp", "lat", None, None), P("dp", "lat", None, None), P(), P(), P())
    out_specs = (P("dp", "lat", None, None), P(), P(), P())
    return jax.shard_map(body, mesh=mesh, in_specs=in_specs, out_specs=out_specs, check_vma=False)
```

```python
import functools
import math

import jax
import jax.numpy as jnp
import numpy as np
from jax import lax
from jax.experimental import pallas as pl
from jax.experimental.pallas import tpu as pltpu
from jax.sharding import PartitionSpec as P

MW = 64
NLAT = 128
NLON = 256
FEAT = 128
HID = 1024
ROWS = 512
BANDS = 64
BLK = 1280
BF = jnp.bfloat16
F32 = jnp.float32
MESH = pl.DeviceIdType.MESH


def split_terms(table):
    high = table.astype(np.float32).astype(np.dtype(BF))
    low = (table - high.astype(np.float64)).astype(np.float32).astype(np.dtype(BF))
    return np.concatenate([high, high, low], axis=1)


@functools.lru_cache(maxsize=None)
def constant_tables():
    lon = np.arange(NLON)
    wave = np.arange(MW)
    angle = 2.0 * math.pi * ((wave[:, None] * lon[None, :]) % NLON) / NLON
    base = np.concatenate([np.cos(angle), -np.sin(angle)], axis=0)
    factor = np.where(wave == 0, 1.0, 2.0)
    analysis = base / NLON
    synthesis = base * np.concatenate([factor, factor])[:, None]
    to_waves = np.stack([split_terms(analysis), split_terms(synthesis)])
    to_grid = np.stack([split_terms(synthesis.T), split_terms(analysis.T)])

    latitude = (np.arange(NLAT) + 0.5) * (math.pi / NLAT) - 0.5 * math.pi
    mu, cosine = np.sin(latitude), np.cos(latitude)
    quad = cosine * (math.pi / NLAT)
    table = np.zeros((MW, MW, NLAT))
    for m in range(MW):
        steps = np.arange(1, m + 1)
        increments = 0.5 * np.log((2.0 * steps + 1.0) / (2.0 * steps))
        current = np.exp(0.5 * math.log(0.5) + increments.sum() + m * np.log(cosine))
        previous, ratio_prev = np.zeros(NLAT), 1.0
        table[m, 0] = current
        for k in range(1, MW - m):
            n = float(m + k)
            ratio = math.sqrt((4.0 * n * n - 1.0) / (n * n - m * m))
            previous, current = current, ratio * (mu * current - previous / ratio_prev)
            ratio_prev = ratio
            table[m, k] = current
    table = np.concatenate([table[:, :, 0::2], table[:, :, 1::2]], axis=2)
    packed = [table[m, : MW - 8 * (m // 8)] for m in range(MW)] + [np.zeros((MW - 8, NLAT))]
    return to_waves, to_grid, np.concatenate(packed).astype(np.float32), quad.astype(np.float32)


def times(table, value):
    high = value.astype(BF)
    low = (value - high.astype(F32)).astype(BF)
    return jnp.dot(table, jnp.concatenate([high, low, high], axis=0), preferred_element_type=F32)


def terms(table):
    high = table.astype(BF)
    low = (table - high.astype(F32)).astype(BF)
    return jnp.concatenate([high, high, low], axis=1)


def nt(a, b):
    return lax.dot_general(a, b, (((1,), (1,)), ((), ())), preferred_element_type=F32)


def tn(a, b):
    return lax.dot_general(a, b, (((0,), (0,)), ((), ())), preferred_element_type=F32)


def spread(send, waves, kind):
    for lat in range(2):
        for part in range(2):
            send[pl.ds(kind * 4 + lat * 2 + part, BANDS, stride=8), :] = waves[
                part * MW : (part + 1) * MW, lat * FEAT : (lat + 1) * FEAT
            ]


def gather_parts(recv, kind):
    return jnp.concatenate(
        [
            jnp.concatenate(
                [recv[pl.ds(kind * 4 + lat * 2 + part, BANDS, stride=8), :] for lat in range(2)],
                axis=1,
            )
            for part in range(2)
        ],
        axis=0,
    )


def kernel(
    state_in, cot_in, w1_in, w2_in, w3_in, tab_in, tf_in, ti_in, quad_in,
    final, total,
    state, cot, w1, w2, w3, tab, tf, ti,
    inward, outward, grads, field, x0, x1, gt, ha0, hb0, da0, db0, ha1, hb1, da1, db1, ga, gb,
    send, recv, core_buf, half_buf, z_buf,
    loads, a2a_send, a2a_recv, core_send, core_recv, rs_send, rs_recv, z_send, z_recv,
):
    me = lax.axis_index("lat")
    dp = lax.axis_index("dp")
    xh, core = dp // 2, lax.rem(dp, 2)
    xl, zy = me // 32, lax.rem(me, 32)
    z, y = zy // 4, lax.rem(zy, 4)
    yh, yl = y // 2, lax.rem(y, 2)
    mate = {"lat": me, "dp": xh * 2 + 1 - core}
    partner = {
        "xa": {"lat": (1 - xl) * 32 + zy, "dp": dp},
        "xb": {"lat": (1 - xl) * 32 + zy, "dp": (1 - xh) * 2 + core},
        "ya": {"lat": xl * 32 + z * 4 + yh * 2 + 1 - yl, "dp": dp},
        "yb": {"lat": xl * 32 + z * 4 + 3 - y, "dp": dp},
    }
    bit = {"xa": lax.rem(xl + xh, 2), "xb": xh, "ya": lax.rem(yl + yh, 2), "yb": yh}

    def partners(act):
        def run(first, width):
            def inner(i, carry):
                for k in range(width):
                    act(lax.rem(me + (first + i * width + k), BANDS))
                return carry

            return inner

        lax.fori_loop(0, 4, run(44, 5), 0)
        lax.fori_loop(0, 6, run(1, 7), 0)
        act(lax.rem(me + 43, BANDS))

    barrier = pltpu.get_barrier_semaphore()
    partners(
        lambda target: pl.semaphore_signal(
            barrier, inc=1, device_id={"lat": target, "dp": dp}, device_id_type=MESH
        )
    )
    for other in (mate, partner["xb"]):
        pl.semaphore_signal(barrier, inc=1, device_id=other, device_id_type=MESH)

    group = me // 8
    first_row = 64 * (8 * group - group * (group - 1) // 2) + lax.rem(me, 8) * (8 - group) * 8
    wanted = {
        "cot": (cot_in, cot), "tf": (tf_in, tf), "state": (state_in, state), "w1": (w1_in, w1),
        "w2": (w2_in, w2), "w3": (w3_in, w3), "ti": (ti_in, ti),
        "tab": (tab_in.at[pl.ds(pl.multiple_of(first_row, 8), MW), :], tab),
    }
    loading = {
        name: pltpu.make_async_copy(a, b, loads.at[i]) for i, (name, (a, b)) in enumerate(wanted.items())
    }
    for c in loading.values():
        c.start()

    def hidden(lat, x, ha, hb, da, db):
        rows = pl.ds(pl.multiple_of(lat * NLON, NLON), NLON)
        mine = x[rows, :]
        for layer in range(2):
            weight, act, slope = ((w1, ha, da), (w2, hb, db))[layer]
            rows_in = mine if layer == 0 else ha[rows, :]
            for n in range(4):
                cols = slice(n * 256, (n + 1) * 256)
                pre = jnp.dot(rows_in, weight[:, cols], preferred_element_type=F32)
                gate = jax.nn.sigmoid(pre)
                out = pre * gate
                act[rows, cols] = out.astype(BF)
                slope[rows, cols] = gate * (1.0 + pre * (1.0 - gate))

    def tendency(lat, source, hb):
        rows = pl.ds(pl.multiple_of(lat * NLON, NLON), NLON)
        tend = jnp.dot(hb[rows, :], w3[...], preferred_element_type=F32)
        field[rows, :] = source[rows, :] + 0.5 * tend

    def backward_b(lat, db):
        rows = pl.ds(pl.multiple_of(lat * NLON, NLON), NLON)
        scaled = gt[rows, :]
        for n in range(4):
            cols = slice(n * 256, (n + 1) * 256)
            gb[rows, cols] = (nt(scaled, w3[cols, :]) * db[rows, cols]).astype(BF)

    def backward_a(lat, da, pulled):
        rows = pl.ds(pl.multiple_of(lat * NLON, NLON), NLON)
        grad_b = gb[rows, :]
        for n in range(4):
            cols = slice(n * 256, (n + 1) * 256)
            ga[rows, cols] = (nt(grad_b, w2[cols, :]) * da[rows, cols]).astype(BF)
        if pulled is not None:
            pulled[rows, :] = pulled[rows, :] + nt(ga[rows, :], w1[...])

    def put(start, value, add, flip=False):
        for half in range(2):
            block = value[:, half * 128 : (half + 1) * 128]
            block = block.T if flip else block
            rows = pl.ds(pl.multiple_of(start + half * BLK, 128), block.shape[0])
            grads[rows, :] = block + grads[rows, :] if add else block

    def some(half, n):
        return pl.ds(pl.multiple_of(half * 512 + n * 256, 256), 256)

    def middle_grads(half, ha, add):
        def run(i, carry):
            left = ha[:, pl.ds(pl.multiple_of(i * 256, 256), 256)]
            for n in range(2):
                put((half * 4 + 2 * n) * BLK + i * 256, tn(left, gb[:, some(half, n)]), add)
            return carry

        lax.fori_loop(0, 4, run, 0)

    def outer_grads(half, x, hb, add):
        for n in range(2):
            start = (half * 4 + 2 * n) * BLK
            put(start + 1024, tn(x[...], ga[:, some(half, n)]), add)
            put(start + 1152, tn(gt[...], hb[:, some(half, n)]), add, True)

    def lanes(ref):
        return jnp.concatenate([ref[0:NLON, :], ref[NLON : 2 * NLON, :]], axis=1)

    quad = jnp.concatenate([jnp.full((1, FEAT), quad_in[2 * me + lat], F32) for lat in range(2)], axis=1)

    def to_waves(ref, kind, out):
        waves = times(tf[kind], lanes(ref))
        spread(out, waves * quad if kind == 0 else waves, kind)

    def to_grid(source, kind):
        value = times(ti[kind], gather_parts(source, kind))
        return value if kind == 0 else value * quad

    def piece(ref, index, device, kind):
        return ref.at[index, pl.ds(pl.multiple_of(device * 8, 8), 8), :].at[pl.ds(4 * kind, 4), :]

    def exchange(index, kind):
        def start(target):
            pltpu.make_async_remote_copy(
                src_ref=piece(send, index, target, kind),
                dst_ref=piece(recv, index, me, kind),
                send_sem=a2a_send.at[2 * index + kind],
                recv_sem=a2a_recv.at[2 * index + kind],
                device_id={"lat": target, "dp": dp},
                device_id_type=MESH,
            ).start()

        partners(start)
        mine = pl.ds(pl.multiple_of(me * 8, 8) + 4 * kind, 4)
        recv[index, mine, :] = send[index, mine, :]

    def bytes_of_all(ref, sem, index, kind):
        half = ref.at[index, pl.ds(0, 4 * (BANDS - 1)), :]
        pltpu.make_async_copy(half, half, sem.at[2 * index + kind]).wait()

    def arrive(index, kind):
        bytes_of_all(recv, a2a_recv, index, kind)

    def legendre_tables():
        degree = me + lax.broadcasted_iota(jnp.int32, (MW, NLAT), 0)
        size = (degree * (degree + 1)).astype(F32)
        damping = jnp.where(degree <= MW - 1, 1.0 / (1.0 + size / (MW * (MW - 1.0))), 0.0)
        poly = tab[...]
        inward[...] = terms(poly * damping)
        outward[...] = terms(poly.T)

    def legendre(source, target, kind):
        value = jnp.concatenate(
            [
                jnp.concatenate(
                    [source[pl.ds(kind * 4 + lat * 2 + part, BANDS, stride=8), :] for lat in range(2)],
                    axis=0,
                )
                for part in range(2)
            ],
            axis=1,
        )
        coeffs = times(inward[...], value)
        back = times(outward[...], coeffs)
        for part in range(2):
            for lat in range(2):
                target[pl.ds(kind * 4 + lat * 2 + part, BANDS, stride=8), :] = back[
                    lat * BANDS : (lat + 1) * BANDS, part * FEAT : (part + 1) * FEAT
                ]

    def turn(index, kind):
        arrive(index, kind)
        legendre(recv.at[index], send.at[index + 1], kind)
        exchange(index + 1, kind)

    def both(step):
        def run(lat, carry):
            step(lat)
            return carry

        lax.fori_loop(0, 2, run, 0)

    for name in ("cot", "tf"):
        loading[name].wait()
    to_waves(cot, 1, send.at[0])
    for name in ("state", "w1", "w2", "w3"):
        loading[name].wait()
    x0[...] = state[...].astype(BF)

    both(lambda lat: hidden(lat, x0, ha0, hb0, da0, db0))
    both(lambda lat: tendency(lat, state, hb0))
    to_waves(field, 0, send.at[0])
    pl.semaphore_wait(barrier, BANDS + 1)
    exchange(0, 0)
    exchange(0, 1)
    for name in ("ti", "tab"):
        loading[name].wait()
    legendre_tables()
    turn(0, 0)
    turn(0, 1)

    halves = [(slice(lat * NLON, (lat + 1) * NLON), slice(lat * FEAT, (lat + 1) * FEAT)) for lat in range(2)]
    arrive(1, 0)
    value = to_grid(recv.at[1], 0)
    for rows, cols in halves:
        field[rows, :] = value[:, cols]
        x1[rows, :] = value[:, cols].astype(BF)
    both(lambda lat: hidden(lat, x1, ha1, hb1, da1, db1))
    arrive(1, 1)
    pulled = to_grid(recv.at[1], 1)
    for rows, cols in halves:
        final[rows, :] = pulled[:, cols]
        gt[rows, :] = (0.5 * pulled[:, cols]).astype(BF)
    both(lambda lat: backward_b(lat, db1))
    both(lambda lat: backward_a(lat, da1, final))
    to_waves(final, 1, send.at[2])
    exchange(2, 1)
    both(lambda lat: tendency(lat, field, hb1))
    to_waves(field, 0, send.at[2])
    exchange(2, 0)
    for half in range(2):
        middle_grads(half, ha1, False)
        outer_grads(half, x1, hb1, False)
    turn(2, 1)
    turn(2, 0)

    arrive(3, 1)
    pulled = to_grid(recv.at[3], 1)
    for rows, cols in halves:
        gt[rows, :] = (0.5 * pulled[:, cols]).astype(BF)
    both(lambda lat: backward_b(lat, db0))

    def tiles(ref, start, count):
        return ref.at[pl.ds(pl.multiple_of(start * 8, 8), count * 8), :]

    def add(start, source, source_start, count):
        width = 20 if count % 20 == 0 else 10 if count % 10 == 0 else 5

        def one(i, carry):
            for j in range(width):
                into = pl.ds(pl.multiple_of((start + i * width + j) * 8, 8), 8)
                rows = pl.ds(pl.multiple_of((source_start + i * width + j) * 8, 8), 8)
                grads[into, :] = grads[into, :] + source[rows, :]
            return carry

        if count == width:
            one(0, 0)
        else:
            lax.fori_loop(0, count // width, one, 0)

    def copy(source, target, send_sem, recv_sem, device):
        return pltpu.make_async_remote_copy(
            src_ref=source, dst_ref=target, send_sem=send_sem, recv_sem=recv_sem,
            device_id=device, device_id_type=MESH,
        )

    order = (
        ("xa", "xb", "ya", "yb"),
        ("xb", "xa", "yb", "ya"),
        ("ya", "yb", "xa", "xb"),
        ("yb", "ya", "xb", "xa"),
    )
    size = 80
    parts = (0, 2, 4, 6, 1, 3, 5, 7)
    starts = {}

    def to_mate(chosen):
        for s in chosen:
            c = copy(
                tiles(grads, (1 - core) * 640 + s * size, size), tiles(core_buf, s * size, size),
                core_send.at[s], core_recv.at[s], mate,
            )
            c.start()
            starts[s] = c

    offset = {s: core * 640 + s * size for s in parts}
    kept = {s: [offset[s]] for s in parts}
    place = 0
    early, late = {}, {}

    def take(entry):
        c, start, base, count = entry
        c.wait_recv()
        add(start, half_buf, base, count)

    def reduce_step(s, step):
        nonlocal place
        count = size >> (step + 1)
        now = kept[s][step]
        if step >= 2:
            take(late[s, step - 2])
        if step == 0:
            starts[s].wait_recv()
        else:
            take(early[s, step - 1])
        if step == 4:
            to_owner(s, lambda c: c.start())
            return
        name = order[s // 2][step]
        keep = now + bit[name] * count
        gone = now + (1 - bit[name]) * count
        kept[s].append(keep)
        if step == 0:
            add(gone, core_buf, s * size + (1 - bit[name]) * count, count)
        if step == 3:
            pieces = [(early, 0, count)]
        else:
            ahead = bit[order[s // 2][step + 1]]
            pieces = [(early, (1 - ahead) * (count // 2), count // 2), (late, ahead * (count // 2), count // 2)]
        for i, (book, at, length) in enumerate(pieces):
            sem = 64 * i + step * 8 + s
            c = copy(
                tiles(grads, gone + at, length), tiles(half_buf, place, length),
                rs_send.at[sem], rs_recv.at[sem], partner[name],
            )
            c.start()
            book[s, step] = (c, keep + at, place, length)
            place += length
        if step == 0:
            add(keep, core_buf, s * size + bit[name] * count, count)

    def along_z(index):
        return {"lat": xl * 32 + index * 4 + y, "dp": dp}

    def to_owner(s, act):
        @pl.when(z != s)
        def _():
            act(
                copy(
                    tiles(grads, kept[s][4], 5), tiles(z_buf, 5 * z, 5),
                    z_send.at[s], z_recv.at[z], along_z(s),
                )
            )

    def from_owner(index, i):
        held = tiles(total, chunk(index), 5)
        return copy(held, held, z_send.at[8 + i], z_recv.at[8 + index], along_z(lax.rem(z + i, 8)))

    middle_grads(1 - core, ha0, True)
    to_mate(parts[:4])
    middle_grads(core, ha0, True)
    both(lambda lat: backward_a(lat, da0, None))
    for s in parts[:4]:
        reduce_step(s, 0)
    outer_grads(1 - core, x0, hb0, True)
    to_mate(parts[4:])
    outer_grads(core, x0, hb0, True)
    for s in parts[4:]:
        reduce_step(s, 0)
    for step in range(1, 5):
        for s in parts:
            reduce_step(s, step)

    def chunk(index):
        start = kept[7][4]
        for s in range(7):
            start = jnp.where(index == s, kept[s][4], start)
        return start

    own = chunk(z)
    arrive(3, 0)
    value = to_grid(recv.at[3], 0)
    for rows, cols in halves:
        final[rows, :] = value[:, cols]
    others = [lax.rem(z + i, 8) for i in range(1, 8)]
    for other in others:
        copy(
            tiles(grads, own, 5), tiles(z_buf, 5 * other, 5), z_send.at[0], z_recv.at[other], along_z(other)
        ).wait_recv()
    for j in range(5):
        rows = pl.ds(pl.multiple_of((own + j) * 8, 8), 8)
        value = grads[rows, :]
        for other in others:
            value = value + z_buf[pl.ds(pl.multiple_of((5 * other + j) * 8, 8), 8), :]
        total[rows, :] = value
    for i in range(1, 8):
        from_owner(z, i).start()
    running = {s: [] for s in parts}
    last = []

    def pass_on(s, step, start, length, sem):
        held = tiles(total, start, length)
        c = copy(held, held, rs_send.at[sem], rs_recv.at[sem], partner[order[s // 2][step]])
        c.start()
        running[s].append((step, c))

    for step in (3, 2, 1, 0, -1):
        for s in parts:
            if step < 3:
                for c in [c for at, c in running[s] if at == step + 1]:
                    c.wait_recv()
            else:

                @pl.when(z != s)
                def _():
                    from_owner(s, 1).wait_recv()

            if step == 3:
                pass_on(s, 3, kept[s][4], 5, 56 + s)
            elif step >= 0:
                half = size >> (step + 2)
                pass_on(s, step, 2 * kept[s][step + 1] + half - kept[s][step + 2], half, 32 + step * 8 + s)
            if step >= 1:
                pass_on(s, step - 1, kept[s][step + 1], size >> (step + 1), 88 + (step - 1) * 8 + s)
            if step <= 0:
                first = kept[s][1] if step == 0 else 2 * kept[s][0] + size // 2 - kept[s][1]
                held = tiles(total, first, size // 2)
                sem = 16 + 8 * step + s
                c = copy(held, held, core_send.at[8 + sem], core_recv.at[8 + sem], mate)
                c.start()
                last.append(c)
    for s in parts:
        to_owner(s, lambda c: c.wait_send())
    for i in range(1, 8):
        from_owner(z, i).wait_send()
    for c in last:
        c.wait_recv()
    for index in range(4):
        for kind in range(2):
            bytes_of_all(send, a2a_send, index, kind)
    for c in [*starts.values(), *[entry[0] for entry in [*early.values(), *late.values()]], *last]:
        c.wait_send()
    for s in parts:
        for _, c in running[s]:
            c.wait_send()


def write_out(final, total, field, first, middle, last, sems):
    copies = [(final, field)]
    for c in range(8):
        cols = pl.ds(c * 128, 128)
        copies.append((total.at[pl.ds(c * BLK, 1024), :], middle.at[:, cols]))
        copies.append((total.at[pl.ds(c * BLK + 1024, 128), :], first.at[:, cols]))
        copies.append((total.at[pl.ds(c * BLK + 1152, 128), :], last.at[cols, :]))
    running = [pltpu.make_async_copy(a, b, sems.at[i]) for i, (a, b) in enumerate(copies)]
    for c in running:
        c.start()
    for c in running:
        c.wait()


def body(state, cotangent, w_first, w_middle, w_last):
    to_waves, to_grid, table, quad = constant_tables()
    hbm = pl.BlockSpec(memory_space=pltpu.HBM)
    vmem = pl.BlockSpec(memory_space=pltpu.VMEM)
    act = pltpu.VMEM((ROWS, HID), BF)
    slope = pltpu.VMEM((ROWS, HID), F32)
    thin = pltpu.VMEM((ROWS, FEAT), BF)
    dma = pltpu.SemaphoreType.DMA
    final, total = pl.pallas_call(
        kernel,
        out_shape=(
            pltpu.VMEM((ROWS, FEAT), F32),
            pltpu.VMEM((8 * BLK, 128), F32),
        ),
        in_specs=[hbm] * 8 + [pl.BlockSpec(memory_space=pltpu.SMEM)],
        out_specs=(vmem, vmem),
        scratch_shapes=[
            pltpu.VMEM((ROWS, FEAT), F32), pltpu.VMEM((ROWS, FEAT), F32),
            pltpu.VMEM((FEAT, HID), BF), pltpu.VMEM((HID, HID), BF), pltpu.VMEM((HID, FEAT), BF),
            pltpu.VMEM((MW, NLAT), F32), pltpu.VMEM(to_waves.shape, BF), pltpu.VMEM(to_grid.shape, BF),
            pltpu.VMEM((MW, 3 * NLAT), BF), pltpu.VMEM((NLAT, 3 * MW), BF),
            pltpu.VMEM((8 * BLK, 128), F32), pltpu.VMEM((ROWS, FEAT), F32), thin, thin, thin,
            act, act, slope, slope, act, act, slope, slope, act, act,
            pltpu.VMEM((4, 8 * BANDS, FEAT), F32), pltpu.VMEM((4, 8 * BANDS, FEAT), F32),
            pltpu.VMEM((640 * 8, 128), F32), pltpu.VMEM((600 * 8, 128), F32),
            pltpu.VMEM((40 * 8, 128), F32),
            dma((8,)), dma((8,)), dma((8,)), dma((32,)), dma((32,)), dma((112,)), dma((112,)), dma((16,)), dma((16,)),
        ],
        compiler_params=pltpu.CompilerParams(
            collective_id=0, has_side_effects=True, vmem_limit_bytes=57 * 1024 * 1024
        ),
        name="spectral_steps",
    )(
        state.reshape(ROWS, FEAT), cotangent.reshape(ROWS, FEAT), w_first, w_middle, w_last,
        jnp.asarray(table), jnp.asarray(to_waves), jnp.asarray(to_grid), jnp.asarray(quad),
    )
    anywhere = pl.BlockSpec(memory_space=pl.ANY)
    field, first, middle, last = pl.pallas_call(
        write_out,
        out_shape=(
            jax.ShapeDtypeStruct((ROWS, FEAT), F32),
            jax.ShapeDtypeStruct((FEAT, HID), F32),
            jax.ShapeDtypeStruct((HID, HID), F32),
            jax.ShapeDtypeStruct((HID, FEAT), F32),
        ),
        in_specs=[vmem] * 2,
        out_specs=(anywhere,) * 4,
        scratch_shapes=[dma((25,))],
        compiler_params=pltpu.CompilerParams(vmem_limit_bytes=8 * 1024 * 1024),
        name="write_out",
    )(final, total)
    return field.reshape(state.shape), first, middle, last


def solution(mesh):
    in_specs = (P("dp", "lat", None, None), P("dp", "lat", None, None), P(), P(), P())
    out_specs = (P("dp", "lat", None, None), P(), P(), P())
    return jax.shard_map(body, mesh=mesh, in_specs=in_specs, out_specs=out_specs, check_vma=False)
```

```python
import functools
import math

import jax
import jax.numpy as jnp
import numpy as np
from jax import lax
from jax.experimental import pallas as pl
from jax.experimental.pallas import tpu as pltpu
from jax.sharding import PartitionSpec as P

MW = 64
NLAT = 128
NLON = 256
FEAT = 128
HID = 1024
ROWS = 512
BANDS = 64
BLK = 1280
BF = jnp.bfloat16
F32 = jnp.float32
MESH = pl.DeviceIdType.MESH


def split_terms(table):
    high = table.astype(np.float32).astype(np.dtype(BF))
    low = (table - high.astype(np.float64)).astype(np.float32).astype(np.dtype(BF))
    return np.concatenate([high, high, low], axis=1)


@functools.lru_cache(maxsize=None)
def constant_tables():
    lon = np.arange(NLON)
    wave = np.arange(MW)
    angle = 2.0 * math.pi * ((wave[:, None] * lon[None, :]) % NLON) / NLON
    base = np.concatenate([np.cos(angle), -np.sin(angle)], axis=0)
    factor = np.where(wave == 0, 1.0, 2.0)
    analysis = base / NLON
    synthesis = base * np.concatenate([factor, factor])[:, None]
    to_waves = np.stack([split_terms(analysis), split_terms(synthesis)])
    to_grid = np.stack([split_terms(synthesis.T), split_terms(analysis.T)])

    latitude = (np.arange(NLAT) + 0.5) * (math.pi / NLAT) - 0.5 * math.pi
    mu, cosine = np.sin(latitude), np.cos(latitude)
    quad = cosine * (math.pi / NLAT)
    table = np.zeros((MW, MW, NLAT))
    for m in range(MW):
        steps = np.arange(1, m + 1)
        increments = 0.5 * np.log((2.0 * steps + 1.0) / (2.0 * steps))
        current = np.exp(0.5 * math.log(0.5) + increments.sum() + m * np.log(cosine))
        previous, ratio_prev = np.zeros(NLAT), 1.0
        table[m, 0] = current
        for k in range(1, MW - m):
            n = float(m + k)
            ratio = math.sqrt((4.0 * n * n - 1.0) / (n * n - m * m))
            previous, current = current, ratio * (mu * current - previous / ratio_prev)
            ratio_prev = ratio
            table[m, k] = current
    table = np.concatenate([table[:, :, 0::2], table[:, :, 1::2]], axis=2)
    packed = [table[m, : MW - 8 * (m // 8)] for m in range(MW)] + [np.zeros((MW - 8, NLAT))]
    return to_waves, to_grid, np.concatenate(packed).astype(np.float32), quad.astype(np.float32)


def times(table, value):
    high = value.astype(BF)
    low = (value - high.astype(F32)).astype(BF)
    return jnp.dot(table, jnp.concatenate([high, low, high], axis=0), preferred_element_type=F32)


def terms(table):
    high = table.astype(BF)
    low = (table - high.astype(F32)).astype(BF)
    return jnp.concatenate([high, high, low], axis=1)


def nt(a, b):
    return lax.dot_general(a, b, (((1,), (1,)), ((), ())), preferred_element_type=F32)


def tn(a, b):
    return lax.dot_general(a, b, (((0,), (0,)), ((), ())), preferred_element_type=F32)


def spread(send, waves, kind):
    for lat in range(2):
        for part in range(2):
            send[pl.ds(kind * 4 + lat * 2 + part, BANDS, stride=8), :] = waves[
                part * MW : (part + 1) * MW, lat * FEAT : (lat + 1) * FEAT
            ]


def gather_parts(recv, kind):
    return jnp.concatenate(
        [
            jnp.concatenate(
                [recv[pl.ds(kind * 4 + lat * 2 + part, BANDS, stride=8), :] for lat in range(2)],
                axis=1,
            )
            for part in range(2)
        ],
        axis=0,
    )


def kernel(
    state_in, cot_in, w1_in, w2_in, w3_in, tab_in, tf_in, ti_in, quad_in,
    final, total,
    state, cot, w1, w2, w3, tab, tf, ti,
    inward, outward, grads, field, x0, x1, gt, ha0, hb0, da0, db0, ha1, hb1, da1, db1, ga, gb,
    send, recv, core_buf, half_buf, z_buf,
    loads, a2a_send, a2a_recv, core_send, core_recv, rs_send, rs_recv, z_send, z_recv,
):
    me = lax.axis_index("lat")
    dp = lax.axis_index("dp")
    xh, core = dp // 2, lax.rem(dp, 2)
    xl, zy = me // 32, lax.rem(me, 32)
    z, y = zy // 4, lax.rem(zy, 4)
    yh, yl = y // 2, lax.rem(y, 2)
    mate = {"lat": me, "dp": xh * 2 + 1 - core}
    partner = {
        "xa": {"lat": (1 - xl) * 32 + zy, "dp": dp},
        "xb": {"lat": (1 - xl) * 32 + zy, "dp": (1 - xh) * 2 + core},
        "ya": {"lat": xl * 32 + z * 4 + yh * 2 + 1 - yl, "dp": dp},
        "yb": {"lat": xl * 32 + z * 4 + 3 - y, "dp": dp},
    }
    bit = {"xa": lax.rem(xl + xh, 2), "xb": xh, "ya": lax.rem(yl + yh, 2), "yb": yh}

    def partners(act):
        def run(first, width):
            def inner(i, carry):
                for k in range(width):
                    act(lax.rem(me + (first + i * width + k), BANDS))
                return carry

            return inner

        lax.fori_loop(0, 4, run(44, 5), 0)
        lax.fori_loop(0, 6, run(1, 7), 0)
        act(lax.rem(me + 43, BANDS))

    barrier = pltpu.get_barrier_semaphore()
    partners(
        lambda target: pl.semaphore_signal(
            barrier, inc=1, device_id={"lat": target, "dp": dp}, device_id_type=MESH
        )
    )
    for other in (mate, partner["xb"]):
        pl.semaphore_signal(barrier, inc=1, device_id=other, device_id_type=MESH)

    group = me // 8
    first_row = 64 * (8 * group - group * (group - 1) // 2) + lax.rem(me, 8) * (8 - group) * 8
    wanted = {
        "cot": (cot_in, cot), "tf": (tf_in, tf), "state": (state_in, state), "w1": (w1_in, w1),
        "w2": (w2_in, w2), "w3": (w3_in, w3), "ti": (ti_in, ti),
        "tab": (tab_in.at[pl.ds(pl.multiple_of(first_row, 8), MW), :], tab),
    }
    loading = {
        name: pltpu.make_async_copy(a, b, loads.at[i]) for i, (name, (a, b)) in enumerate(wanted.items())
    }
    for c in loading.values():
        c.start()

    def hidden(lat, x, ha, hb, da, db):
        rows = pl.ds(pl.multiple_of(lat * NLON, NLON), NLON)
        mine = x[rows, :]
        for layer in range(2):
            weight, act, slope = ((w1, ha, da), (w2, hb, db))[layer]
            rows_in = mine if layer == 0 else ha[rows, :]
            for n in range(4):
                cols = slice(n * 256, (n + 1) * 256)
                pre = jnp.dot(rows_in, weight[:, cols], preferred_element_type=F32)
                gate = jax.nn.sigmoid(pre)
                out = pre * gate
                act[rows, cols] = out.astype(BF)
                slope[rows, cols] = gate * (1.0 + pre * (1.0 - gate))

    def tendency(lat, source, hb):
        rows = pl.ds(pl.multiple_of(lat * NLON, NLON), NLON)
        tend = jnp.dot(hb[rows, :], w3[...], preferred_element_type=F32)
        field[rows, :] = source[rows, :] + 0.5 * tend

    def backward_b(lat, db):
        rows = pl.ds(pl.multiple_of(lat * NLON, NLON), NLON)
        scaled = gt[rows, :]
        for n in range(4):
            cols = slice(n * 256, (n + 1) * 256)
            gb[rows, cols] = (nt(scaled, w3[cols, :]) * db[rows, cols]).astype(BF)

    def backward_a(lat, da, pulled):
        rows = pl.ds(pl.multiple_of(lat * NLON, NLON), NLON)
        grad_b = gb[rows, :]
        for n in range(4):
            cols = slice(n * 256, (n + 1) * 256)
            ga[rows, cols] = (nt(grad_b, w2[cols, :]) * da[rows, cols]).astype(BF)
        if pulled is not None:
            pulled[rows, :] = pulled[rows, :] + nt(ga[rows, :], w1[...])

    def put(start, value, add, flip=False):
        for half in range(2):
            block = value[:, half * 128 : (half + 1) * 128]
            block = block.T if flip else block
            rows = pl.ds(pl.multiple_of(start + half * BLK, 128), block.shape[0])
            grads[rows, :] = block + grads[rows, :] if add else block

    def some(half, n):
        return pl.ds(pl.multiple_of(half * 512 + n * 256, 256), 256)

    def middle_grads(half, ha, add):
        def run(i, carry):
            left = ha[:, pl.ds(pl.multiple_of(i * 256, 256), 256)]
            for n in range(2):
                put((half * 4 + 2 * n) * BLK + i * 256, tn(left, gb[:, some(half, n)]), add)
            return carry

        lax.fori_loop(0, 4, run, 0)

    def outer_grads(half, x, hb, add):
        for n in range(2):
            start = (half * 4 + 2 * n) * BLK
            put(start + 1024, tn(x[...], ga[:, some(half, n)]), add)
            put(start + 1152, tn(gt[...], hb[:, some(half, n)]), add, True)

    def lanes(ref):
        return jnp.concatenate([ref[0:NLON, :], ref[NLON : 2 * NLON, :]], axis=1)

    quad = jnp.concatenate([jnp.full((1, FEAT), quad_in[2 * me + lat], F32) for lat in range(2)], axis=1)

    def to_waves(ref, kind, out):
        waves = times(tf[kind], lanes(ref))
        spread(out, waves * quad if kind == 0 else waves, kind)

    def to_grid(source, kind):
        value = times(ti[kind], gather_parts(source, kind))
        return value if kind == 0 else value * quad

    def piece(ref, index, device, kind):
        return ref.at[index, pl.ds(pl.multiple_of(device * 8, 8), 8), :].at[pl.ds(4 * kind, 4), :]

    def exchange(index, kind):
        def start(target):
            pltpu.make_async_remote_copy(
                src_ref=piece(send, index, target, kind),
                dst_ref=piece(recv, index, me, kind),
                send_sem=a2a_send.at[2 * index + kind],
                recv_sem=a2a_recv.at[2 * index + kind],
                device_id={"lat": target, "dp": dp},
                device_id_type=MESH,
            ).start()

        partners(start)
        mine = pl.ds(pl.multiple_of(me * 8, 8) + 4 * kind, 4)
        recv[index, mine, :] = send[index, mine, :]

    def bytes_of_all(ref, sem, index, kind):
        half = ref.at[index, pl.ds(0, 4 * (BANDS - 1)), :]
        pltpu.make_async_copy(half, half, sem.at[2 * index + kind]).wait()

    def arrive(index, kind):
        bytes_of_all(recv, a2a_recv, index, kind)

    def legendre_tables():
        degree = me + lax.broadcasted_iota(jnp.int32, (MW, NLAT), 0)
        size = (degree * (degree + 1)).astype(F32)
        damping = jnp.where(degree <= MW - 1, 1.0 / (1.0 + size / (MW * (MW - 1.0))), 0.0)
        poly = tab[...]
        inward[...] = terms(poly * damping)
        outward[...] = terms(poly.T)

    def legendre(source, target, kind):
        value = jnp.concatenate(
            [
                jnp.concatenate(
                    [source[pl.ds(kind * 4 + lat * 2 + part, BANDS, stride=8), :] for lat in range(2)],
                    axis=0,
                )
                for part in range(2)
            ],
            axis=1,
        )
        coeffs = times(inward[...], value)
        back = times(outward[...], coeffs)
        for part in range(2):
            for lat in range(2):
                target[pl.ds(kind * 4 + lat * 2 + part, BANDS, stride=8), :] = back[
                    lat * BANDS : (lat + 1) * BANDS, part * FEAT : (part + 1) * FEAT
                ]

    def turn(index, kind):
        arrive(index, kind)
        legendre(recv.at[index], send.at[index + 1], kind)
        exchange(index + 1, kind)

    def both(step):
        def run(lat, carry):
            step(lat)
            return carry

        lax.fori_loop(0, 2, run, 0)

    for name in ("cot", "tf"):
        loading[name].wait()
    to_waves(cot, 1, send.at[0])
    for name in ("state", "w1", "w2", "w3"):
        loading[name].wait()
    x0[...] = state[...].astype(BF)

    both(lambda lat: hidden(lat, x0, ha0, hb0, da0, db0))
    both(lambda lat: tendency(lat, state, hb0))
    to_waves(field, 0, send.at[0])
    pl.semaphore_wait(barrier, BANDS + 1)
    exchange(0, 0)
    exchange(0, 1)
    for name in ("ti", "tab"):
        loading[name].wait()
    legendre_tables()
    turn(0, 0)
    turn(0, 1)

    halves = [(slice(lat * NLON, (lat + 1) * NLON), slice(lat * FEAT, (lat + 1) * FEAT)) for lat in range(2)]
    arrive(1, 0)
    value = to_grid(recv.at[1], 0)
    for rows, cols in halves:
        field[rows, :] = value[:, cols]
        x1[rows, :] = value[:, cols].astype(BF)
    both(lambda lat: hidden(lat, x1, ha1, hb1, da1, db1))
    arrive(1, 1)
    pulled = to_grid(recv.at[1], 1)
    for rows, cols in halves:
        final[rows, :] = pulled[:, cols]
        gt[rows, :] = (0.5 * pulled[:, cols]).astype(BF)
    both(lambda lat: backward_b(lat, db1))
    both(lambda lat: backward_a(lat, da1, final))
    to_waves(final, 1, send.at[2])
    exchange(2, 1)
    both(lambda lat: tendency(lat, field, hb1))
    to_waves(field, 0, send.at[2])
    exchange(2, 0)
    for half in range(2):
        middle_grads(half, ha1, False)
        outer_grads(half, x1, hb1, False)
    turn(2, 1)
    turn(2, 0)

    arrive(3, 1)
    pulled = to_grid(recv.at[3], 1)
    for rows, cols in halves:
        gt[rows, :] = (0.5 * pulled[:, cols]).astype(BF)
    both(lambda lat: backward_b(lat, db0))

    def tiles(ref, start, count):
        return ref.at[pl.ds(pl.multiple_of(start * 8, 8), count * 8), :]

    def add(start, source, source_start, count):
        width = 20 if count % 20 == 0 else 10 if count % 10 == 0 else 5

        def one(i, carry):
            for j in range(width):
                into = pl.ds(pl.multiple_of((start + i * width + j) * 8, 8), 8)
                rows = pl.ds(pl.multiple_of((source_start + i * width + j) * 8, 8), 8)
                grads[into, :] = grads[into, :] + source[rows, :]
            return carry

        if count == width:
            one(0, 0)
        else:
            lax.fori_loop(0, count // width, one, 0)

    def copy(source, target, send_sem, recv_sem, device):
        return pltpu.make_async_remote_copy(
            src_ref=source, dst_ref=target, send_sem=send_sem, recv_sem=recv_sem,
            device_id=device, device_id_type=MESH,
        )

    order = (
        ("xa", "xb", "ya", "yb"),
        ("xb", "xa", "yb", "ya"),
        ("ya", "yb", "xa", "xb"),
        ("yb", "ya", "xb", "xa"),
    )
    size = 80
    parts = (0, 2, 4, 6, 1, 3, 5, 7)
    starts = {}

    def to_mate(chosen):
        for s in chosen:
            c = copy(
                tiles(grads, (1 - core) * 640 + s * size, size), tiles(core_buf, s * size, size),
                core_send.at[s], core_recv.at[s], mate,
            )
            c.start()
            starts[s] = c

    offset = {s: core * 640 + s * size for s in parts}
    kept = {s: [offset[s]] for s in parts}
    place = 0
    early, late = {}, {}

    def take(entry):
        c, start, base, count = entry
        c.wait_recv()
        add(start, half_buf, base, count)

    def reduce_step(s, step):
        nonlocal place
        count = size >> (step + 1)
        now = kept[s][step]
        if step >= 2:
            take(late[s, step - 2])
        if step == 0:
            starts[s].wait_recv()
        else:
            take(early[s, step - 1])
        if step == 4:
            to_owner(s, lambda c: c.start())
            return
        name = order[s // 2][step]
        keep = now + bit[name] * count
        gone = now + (1 - bit[name]) * count
        kept[s].append(keep)
        if step == 0:
            add(gone, core_buf, s * size + (1 - bit[name]) * count, count)
        if step == 3:
            pieces = [(early, 0, count)]
        else:
            ahead = bit[order[s // 2][step + 1]]
            pieces = [(early, (1 - ahead) * (count // 2), count // 2), (late, ahead * (count // 2), count // 2)]
        for i, (book, at, length) in enumerate(pieces):
            sem = 64 * i + step * 8 + s
            c = copy(
                tiles(grads, gone + at, length), tiles(half_buf, place, length),
                rs_send.at[sem], rs_recv.at[sem], partner[name],
            )
            c.start()
            book[s, step] = (c, keep + at, place, length)
            place += length
        if step == 0:
            add(keep, core_buf, s * size + bit[name] * count, count)

    def along_z(index):
        return {"lat": xl * 32 + index * 4 + y, "dp": dp}

    def to_owner(s, act):
        @pl.when(z != s)
        def _():
            act(
                copy(
                    tiles(grads, kept[s][4], 5), tiles(z_buf, 5 * z, 5),
                    z_send.at[s], z_recv.at[z], along_z(s),
                )
            )

    def from_owner(index, i):
        held = tiles(total, chunk(index), 5)
        return copy(held, held, z_send.at[8 + i], z_recv.at[8 + index], along_z(lax.rem(z + i, 8)))

    middle_grads(1 - core, ha0, True)
    to_mate(parts[:4])
    middle_grads(core, ha0, True)
    both(lambda lat: backward_a(lat, da0, None))
    for s in parts[:4]:
        reduce_step(s, 0)
    outer_grads(1 - core, x0, hb0, True)
    to_mate(parts[4:])
    outer_grads(core, x0, hb0, True)
    for s in parts[4:]:
        reduce_step(s, 0)
    for step in range(1, 5):
        for s in parts:
            reduce_step(s, step)

    def chunk(index):
        start = kept[7][4]
        for s in range(7):
            start = jnp.where(index == s, kept[s][4], start)
        return start

    own = chunk(z)
    arrive(3, 0)
    value = to_grid(recv.at[3], 0)
    for rows, cols in halves:
        final[rows, :] = value[:, cols]
    others = [lax.rem(z + i, 8) for i in range(1, 8)]
    for other in others:
        copy(
            tiles(grads, own, 5), tiles(z_buf, 5 * other, 5), z_send.at[0], z_recv.at[other], along_z(other)
        ).wait_recv()
    for j in range(5):
        rows = pl.ds(pl.multiple_of((own + j) * 8, 8), 8)
        value = grads[rows, :]
        for other in others:
            value = value + z_buf[pl.ds(pl.multiple_of((5 * other + j) * 8, 8), 8), :]
        total[rows, :] = value
    for i in range(1, 8):
        from_owner(z, i).start()
    running = {s: [] for s in parts}
    last = []

    def pass_on(s, step, start, length, sem):
        held = tiles(total, start, length)
        c = copy(held, held, rs_send.at[sem], rs_recv.at[sem], partner[order[s // 2][step]])
        c.start()
        running[s].append((step, c))

    def to_other_core(start, length, sem):
        held = tiles(total, start, length)
        c = copy(held, held, core_send.at[sem], core_recv.at[sem], mate)
        c.start()
        last.append(c)

    for step in (3, 2, 1, 0):
        for s in parts:
            if step < 3:
                for c in [c for at, c in running[s] if at == step + 1]:
                    c.wait_recv()
            else:

                @pl.when(z != s)
                def _():
                    from_owner(s, 1).wait_recv()

            if step == 3:
                pass_on(s, 3, kept[s][4], 5, 56 + s)
            elif step >= 0:
                half = size >> (step + 2)
                pass_on(s, step, 2 * kept[s][step + 1] + half - kept[s][step + 2], half, 32 + step * 8 + s)
            if step >= 1:
                pass_on(s, step - 1, kept[s][step + 1], size >> (step + 1), 88 + (step - 1) * 8 + s)
            if step == 0:
                to_other_core(kept[s][1], size // 2, 16 + s)

    for i in range(2):
        for s in parts:
            [c for at, c in running[s] if at == 0][i].wait_recv()
            other = 2 * kept[s][0] + size // 2 - kept[s][1]
            ahead = kept[s][2] - kept[s][1]
            at = other + (ahead if i == 0 else size // 4 - ahead)
            to_other_core(at, size // 4, 24 + 8 * i + s)
    for s in parts:
        to_owner(s, lambda c: c.wait_send())
    for i in range(1, 8):
        from_owner(z, i).wait_send()
    for c in last:
        c.wait_recv()
    for index in range(4):
        for kind in range(2):
            bytes_of_all(send, a2a_send, index, kind)
    for c in [*starts.values(), *[entry[0] for entry in [*early.values(), *late.values()]], *last]:
        c.wait_send()
    for s in parts:
        for _, c in running[s]:
            c.wait_send()


def write_out(final, total, field, first, middle, last, sems):
    copies = [(final, field)]
    for c in range(8):
        cols = pl.ds(c * 128, 128)
        copies.append((total.at[pl.ds(c * BLK, 1024), :], middle.at[:, cols]))
        copies.append((total.at[pl.ds(c * BLK + 1024, 128), :], first.at[:, cols]))
        copies.append((total.at[pl.ds(c * BLK + 1152, 128), :], last.at[cols, :]))
    running = [pltpu.make_async_copy(a, b, sems.at[i]) for i, (a, b) in enumerate(copies)]
    for c in running:
        c.start()
    for c in running:
        c.wait()


def body(state, cotangent, w_first, w_middle, w_last):
    to_waves, to_grid, table, quad = constant_tables()
    hbm = pl.BlockSpec(memory_space=pltpu.HBM)
    vmem = pl.BlockSpec(memory_space=pltpu.VMEM)
    act = pltpu.VMEM((ROWS, HID), BF)
    slope = pltpu.VMEM((ROWS, HID), F32)
    thin = pltpu.VMEM((ROWS, FEAT), BF)
    dma = pltpu.SemaphoreType.DMA
    final, total = pl.pallas_call(
        kernel,
        out_shape=(
            pltpu.VMEM((ROWS, FEAT), F32),
            pltpu.VMEM((8 * BLK, 128), F32),
        ),
        in_specs=[hbm] * 8 + [pl.BlockSpec(memory_space=pltpu.SMEM)],
        out_specs=(vmem, vmem),
        scratch_shapes=[
            pltpu.VMEM((ROWS, FEAT), F32), pltpu.VMEM((ROWS, FEAT), F32),
            pltpu.VMEM((FEAT, HID), BF), pltpu.VMEM((HID, HID), BF), pltpu.VMEM((HID, FEAT), BF),
            pltpu.VMEM((MW, NLAT), F32), pltpu.VMEM(to_waves.shape, BF), pltpu.VMEM(to_grid.shape, BF),
            pltpu.VMEM((MW, 3 * NLAT), BF), pltpu.VMEM((NLAT, 3 * MW), BF),
            pltpu.VMEM((8 * BLK, 128), F32), pltpu.VMEM((ROWS, FEAT), F32), thin, thin, thin,
            act, act, slope, slope, act, act, slope, slope, act, act,
            pltpu.VMEM((4, 8 * BANDS, FEAT), F32), pltpu.VMEM((4, 8 * BANDS, FEAT), F32),
            pltpu.VMEM((640 * 8, 128), F32), pltpu.VMEM((600 * 8, 128), F32),
            pltpu.VMEM((40 * 8, 128), F32),
            dma((8,)), dma((8,)), dma((8,)), dma((40,)), dma((40,)), dma((112,)), dma((112,)), dma((16,)), dma((16,)),
        ],
        compiler_params=pltpu.CompilerParams(
            collective_id=0, has_side_effects=True, vmem_limit_bytes=57 * 1024 * 1024
        ),
        name="spectral_steps",
    )(
        state.reshape(ROWS, FEAT), cotangent.reshape(ROWS, FEAT), w_first, w_middle, w_last,
        jnp.asarray(table), jnp.asarray(to_waves), jnp.asarray(to_grid), jnp.asarray(quad),
    )
    anywhere = pl.BlockSpec(memory_space=pl.ANY)
    field, first, middle, last = pl.pallas_call(
        write_out,
        out_shape=(
            jax.ShapeDtypeStruct((ROWS, FEAT), F32),
            jax.ShapeDtypeStruct((FEAT, HID), F32),
            jax.ShapeDtypeStruct((HID, HID), F32),
            jax.ShapeDtypeStruct((HID, FEAT), F32),
        ),
        in_specs=[vmem] * 2,
        out_specs=(anywhere,) * 4,
        scratch_shapes=[dma((25,))],
        compiler_params=pltpu.CompilerParams(vmem_limit_bytes=8 * 1024 * 1024),
        name="write_out",
    )(final, total)
    return field.reshape(state.shape), first, middle, last


def solution(mesh):
    in_specs = (P("dp", "lat", None, None), P("dp", "lat", None, None), P(), P(), P())
    out_specs = (P("dp", "lat", None, None), P(), P(), P())
    return jax.shard_map(body, mesh=mesh, in_specs=in_specs, out_specs=out_specs, check_vma=False)
```
